32 devices in a mesh: io: 16 (over z, x, core), rep: 2 (over y).
Axes of the slice: x: 2, y: 2, z: 4, core: 2. Of those that a mesh axis runs over, the one named last changes fastest.
Arguments:
- snapshots: float32 [49152, 2048], P(('rep', 'io')), parts along dimension 0, may hold values from -6 to 6
Outputs:
- coefficients: float32 [32, 256, 2048], P('rep', None, 'io'), parts along dimension 0
- resid_var: float32 [512, 2048], P('rep', 'io'), parts along dimension 0
The draws below stay inside these ranges and needn't reach their ends.
There are 2 independent parts, one for each index of `rep`. The reference program is written for one: setup_inputs(seed, part) draws one part's arguments, and reference() takes and returns one part's arrays. A program takes and returns all parts, laid end to end along the dimension named above; each array names one. Nothing has to cross between parts.
All inputs are finite; a program needn't handle non-finite values.
Results may differ from the reference program's by a relative error of at most 0.000071.
Values sent between devices are 32-bit elements; how exact they have to be, the bound alone decides.
A program may use at most 128 MiB of HBM per device.

```python
import jax
import jax.numpy as jnp
from jax import lax

TIMES = 96
HARM = 16
LAT = 256
LON = 2048


def level_of(own_key, dims, cuts, low, top_value):
    def one(axis_at, parts):
        heights = jax.random.uniform(jax.random.fold_in(jax.random.fold_in(own_key, 6), axis_at), (parts,), jnp.float32, low / len(cuts), top_value / len(cuts))
        return jnp.repeat(jnp.exp(heights), dims[axis_at] // parts).reshape((-1,) + (1,) * (len(dims) - axis_at - 1))

    gain = one(*cuts[0])
    for cut in cuts[1:]:
        gain = gain * one(*cut)
    return gain


def normal_values(rng, dims, deviation, bound, cuts=(), dtype=jnp.bfloat16):
    array = deviation * jax.random.normal(rng, dims, jnp.float32)
    if cuts:
        array = array * level_of(rng, dims, cuts, -0.22, 0.18)
    return jnp.clip(array, -bound, bound).astype(dtype)


def setup_inputs(seed: int = 0, part: int = 0) -> dict:
    arg_keys = jax.random.split(jax.random.key(seed), 2)
    part_splits = jax.random.split(jax.random.fold_in(arg_keys[1], part), 2)
    snapshots = normal_values(part_splits[0], (TIMES * LAT, LON), 1.0, 6.0, ((0, 16),), jnp.float32)
    return {"snapshots": snapshots}


def basis_matrix(times):
    steps = jnp.arange(times).astype(jnp.float32)
    columns = [jnp.ones_like(steps), (steps - (times - 1) / 2.0) / (times / 2.0)]
    for harmonic in range(1, 7):
        columns.append(jnp.cos(2.0 * jnp.pi * harmonic * steps / 12.0))
    for harmonic in range(1, 6):
        columns.append(jnp.sin(2.0 * jnp.pi * harmonic * steps / 12.0))
    columns.append(jnp.cos(2.0 * jnp.pi * steps / times))
    columns.append(jnp.sin(2.0 * jnp.pi * steps / times))
    columns.append(jnp.cos(4.0 * jnp.pi * steps / times))
    return jnp.stack(columns, axis=1)

def projector_of(basis):
    gram = jnp.dot(basis.T, basis, precision=lax.Precision.HIGHEST)
    factor = jnp.linalg.cholesky(gram)
    middle = lax.linalg.triangular_solve(factor, basis.T, left_side=True, lower=True)
    return lax.linalg.triangular_solve(factor, middle, left_side=True, lower=True, transpose_a=True)

def reference(snapshots):
    series = snapshots.reshape(TIMES, LAT * LON)
    basis = basis_matrix(TIMES)
    projector = projector_of(basis)
    coeffs = jnp.dot(projector, series, precision=lax.Precision.HIGHEST)
    fitted = jnp.dot(basis, coeffs, precision=lax.Precision.HIGHEST)
    resid = series - fitted
    variance = jnp.mean(resid * resid, axis=0)
    return (coeffs.reshape(HARM, LAT, LON), variance.reshape(LAT, LON))
```

```python
import functools

import jax
import jax.numpy as jnp
import numpy as np
from jax import lax
from jax.experimental import pallas as pl
from jax.experimental.pallas import tpu as pltpu
from jax.sharding import PartitionSpec as P

TIMES = 96
HARM = 16
MONTHS = 12
SPAN = 24
CHAIN = TIMES // SPAN
SLOW = 4
SUMS = MONTHS + SLOW + 1
LANES = 128
ROWS = 8
AHEAD = 4
SKEW = 3
MESH = pl.DeviceIdType.MESH


def schedule():
    far = [[to for to in sorted(range(CHAIN), key=lambda to: -abs(to - at)) if to != at] for at in range(CHAIN)]
    orders = [blocks + [at] for at, blocks in enumerate(far)]
    added = []
    for at in range(CHAIN):
        lags, near = {}, min(at, CHAIN - 1 - at)
        for to in far[at]:
            side = [other for other in far[at] if (other > at) == (to > at)]
            lags[to] = SKEW * side.index(to)
        lags[at] = SKEW * (CHAIN - 2)
        added.append(lags)
    up, down = {}, {}
    for to in range(CHAIN):
        for at in range(to + 1):
            up[at, to] = added[0][to] if at == 0 else max(added[at][to], up[at - 1, to] + 1)
        for at in range(CHAIN - 1, to - 1, -1):
            down[at, to] = added[at][to] if at == CHAIN - 1 else max(added[at][to], down[at + 1, to] + 1)
    hold = max(
        [up[at + 1, to] - up[at, to] for at, to in up if at < to]
        + [down[at - 1, to] - down[at, to] for at, to in down if at > to]
    )
    close = [max(up[at, at], down[at, at]) for at in range(CHAIN)]
    last = max([lag for (at, to), lag in up.items() if at < to] + [lag for (at, to), lag in down.items() if at > to])
    return orders, added, up, down, close, hold, last


ORDERS, ADDED, UP, DOWN, CLOSE, HOLD, LAST_SENT = schedule()
LAST_ADDED = max(max(lags.values()) for lags in ADDED)
RAW_SLOTS = AHEAD + 2
BOX_SLOTS = HOLD + 4


def fit_constants():
    steps = np.arange(TIMES, dtype=np.float64)
    slow = np.stack(
        [
            (steps - (TIMES - 1) / 2.0) / (TIMES / 2.0),
            np.cos(2.0 * np.pi * steps / TIMES),
            np.sin(2.0 * np.pi * steps / TIMES),
            np.cos(4.0 * np.pi * steps / TIMES),
        ],
        axis=1,
    )
    month = np.arange(MONTHS, dtype=np.float64)
    angles = 2.0 * np.pi * month / MONTHS
    periodic = [np.cos(j * angles) for j in range(7)] + [np.sin(j * angles) for j in range(1, 6)]
    unmix = np.linalg.inv(np.stack(periodic, axis=1))
    years = TIMES // MONTHS
    cross = slow.reshape(years, MONTHS, SLOW).sum(axis=0)
    inner = np.linalg.inv(slow.T @ slow - cross.T @ cross / years)
    return slow, cross, inner, unmix, years


def dot(weights, values):
    total = None
    for weight, value in zip(weights, values):
        term = value * np.float32(weight)
        total = term if total is None else total + term
    return total


def finish(sums):
    _, cross, inner, unmix, years = fit_constants()
    by_month, moments, squares = sums[:MONTHS], sums[MONTHS : MONTHS + SLOW], sums[-1]
    reduced = [moments[k] - dot(cross[:, k] / years, by_month) for k in range(SLOW)]
    slow = [dot(inner[k], reduced) for k in range(SLOW)]
    level = [(by_month[m] - dot(cross[m], slow)) * np.float32(1.0 / years) for m in range(MONTHS)]
    explained = slow[0] * moments[0]
    for k in range(1, SLOW):
        explained = explained + slow[k] * moments[k]
    for m in range(MONTHS):
        explained = explained + level[m] * by_month[m]
    half = MONTHS // 2
    even = [level[0]] + [level[m] + level[MONTHS - m] for m in range(1, half)] + [level[half]]
    odd = [level[m] - level[MONTHS - m] for m in range(1, half)]
    cosines = [dot(unmix[j, : half + 1], even) for j in range(half + 1)]
    sines = [dot(unmix[half + j, 1:half], odd) for j in range(1, half)]
    coeffs = [cosines[0], slow[0]] + cosines[1:] + sines + slow[1:]
    return coeffs, (squares - explained) * np.float32(1.0 / TIMES)


def kernel(
    groups, lat, local_rows,
    field, coeff_out, var_out,
    raw, part, below, above,
    raw_send, raw_recv, part_send, box_recv, member_free, box_free,
):
    members = groups // CHAIN
    chunks = lat // ROWS
    me = lax.axis_index("io")
    link, member = me // members, lax.rem(me, members)
    device = lambda at, who: {"io": at * members + who}

    span = fit_constants()[0][:SPAN]
    offset = link.astype(jnp.float32) * np.float32(SPAN / (TIMES / 2.0))
    quarter = lambda at: (link == at).astype(jnp.float32)
    turn_cos, turn_sin = quarter(0) - quarter(2), quarter(1) - quarter(3)
    flip = quarter(0) - quarter(1) + quarter(2) - quarter(3)

    def by_link(values):
        return sum((link == at).astype(jnp.int32) * values[at] for at in range(CHAIN))

    barrier = pltpu.get_barrier_semaphore()
    for step in range(1, members):
        other = lax.rem(member + step, members)
        pl.semaphore_signal(barrier, inc=1, device_id=device(link, other), device_id_type=MESH)

    @pl.when(link > 0)
    def _():
        pl.semaphore_signal(barrier, inc=1, device_id=device(link - 1, member), device_id_type=MESH)

    @pl.when(link < CHAIN - 1)
    def _():
        pl.semaphore_signal(barrier, inc=1, device_id=device(link + 1, member), device_id_type=MESH)

    ends = (link == 0).astype(jnp.int32) + (link == CHAIN - 1).astype(jnp.int32)
    pl.semaphore_wait(barrier, members + 1 - ends)

    def spread_rows(chunk, to, row, count, time):
        for step in list(range(1, members)) + [0]:
            other = lax.rem(member + step, members)
            lon = pl.multiple_of((to * members + other) * LANES, LANES)
            if count is None:
                src = field.at[pl.ds(row, ROWS), pl.ds(lon, LANES)]
                dst = raw.at[chunk, to, time]
            else:
                src = field.at[:, pl.ds(row, ROWS), pl.ds(lon, LANES)]
                dst = raw.at[chunk, to, pl.ds(time, count)]
            arrived = raw_recv.at[lax.rem(chunk, RAW_SLOTS), to]
            if step == 0:
                pltpu.make_async_copy(src, dst, arrived).start()
            else:
                pltpu.make_async_remote_copy(
                    src_ref=src, dst_ref=dst, send_sem=raw_send, recv_sem=arrived,
                    device_id=device(link, other), device_id_type=MESH,
                ).start()

    def spread_block(chunk, to):
        if local_rows % lat == 0:
            count = local_rows // lat
            spread_rows(chunk, to, pl.multiple_of(chunk * ROWS, ROWS), count, member * count)
        else:
            first = member * local_rows
            for extra in range(local_rows // lat + 2):
                time = first // lat + extra
                row = time * lat + chunk * ROWS - first

                @pl.when((row >= 0) & (row < local_rows))
                def _():
                    spread_rows(chunk, to, pl.multiple_of(row, ROWS), None, time)

    def each(step, act):
        for rank in range(CHAIN):
            lag = by_link([ADDED[at][ORDERS[at][rank]] for at in range(CHAIN)])

            @pl.when((step >= lag) & (step < chunks + lag))
            def _():
                act(step - lag, by_link([ORDERS[at][rank] for at in range(CHAIN)]))

    spread_steps = chunks + LAST_ADDED

    def spread(step):
        @pl.when((step >= RAW_SLOTS) & (step < spread_steps))
        def _():
            for away in range(1, members):
                pl.semaphore_wait(member_free.at[away], 1)

        each(step, spread_block)

    def free_members(step):
        @pl.when(step + RAW_SLOTS < spread_steps)
        def _():
            for away in range(1, members):
                other = lax.rem(member + away, members)
                pl.semaphore_signal(
                    member_free.at[members - away], inc=1, device_id=device(link, other), device_id_type=MESH
                )

    send_steps, slack = chunks + LAST_SENT, BOX_SLOTS - HOLD

    def await_boxes(step):
        for up in (True, False):

            @pl.when((link < CHAIN - 1 if up else link > 0) & (step >= slack) & (step < send_steps))
            def _():
                pl.semaphore_wait(box_free.at[0 if up else 1], 1)

    def free_boxes(step):
        for up in (True, False):

            @pl.when((link > 0 if up else link < CHAIN - 1) & (step + slack < send_steps))
            def _():
                pl.semaphore_signal(
                    box_free.at[0 if up else 1], inc=1,
                    device_id=device(link - 1 if up else link + 1, member), device_id_type=MESH,
                )

    def box_sem(chunk, to, up, at):
        where = to if up else to + (to == at).astype(jnp.int32) * (CHAIN - to)
        return box_recv.at[lax.rem(chunk, BOX_SLOTS), where]

    def send(chunk, to, up):
        at = link + 1 if up else link - 1
        pltpu.make_async_remote_copy(
            src_ref=part.at[chunk, to],
            dst_ref=(below if up else above).at[chunk, to],
            send_sem=part_send,
            recv_sem=box_sem(chunk, to, up, at),
            device_id=device(at, member),
            device_id_type=MESH,
        ).start()

    def arrive(chunk, to, up):
        box = below if up else above
        pltpu.make_async_copy(box.at[chunk, to], box.at[chunk, to], box_sem(chunk, to, up, link)).wait()
        for k in range(SUMS):
            part[chunk, to, k] = part[chunk, to, k] + box[chunk, to, k]

    def add_up(chunk, to):
        pltpu.make_async_copy(
            raw.at[chunk, to], raw.at[chunk, to], raw_recv.at[lax.rem(chunk, RAW_SLOTS), to]
        ).wait()
        local = [None] * (SLOW + 1)
        whole = None
        for month in range(MONTHS):
            kept = None
            for time in range(month, SPAN, MONTHS):
                value = raw[chunk, to, time]
                kept = value if kept is None else kept + value
                terms = [value * np.float32(span[time, k]) for k in range(SLOW)] + [value * value]
                local = [term if own is None else own + term for own, term in zip(local, terms)]
            part[chunk, to, month] = kept
            whole = kept if whole is None else whole + kept
        trend, cosine, sine, double, squares = local
        part[chunk, to, MONTHS] = trend + whole * offset
        part[chunk, to, MONTHS + 1] = cosine * turn_cos - sine * turn_sin
        part[chunk, to, MONTHS + 2] = cosine * turn_sin + sine * turn_cos
        part[chunk, to, MONTHS + 3] = double * flip
        part[chunk, to, MONTHS + 4] = squares

        @pl.when((link == 0) & (to > 0))
        def _():
            send(chunk, to, True)

        @pl.when((link == CHAIN - 1) & (to < CHAIN - 1))
        def _():
            send(chunk, to, False)

    def relay(step):
        for at in range(1, CHAIN - 1):
            for to in range(CHAIN):
                if to == at:
                    continue
                lag = UP[at, to] if to > at else DOWN[at, to]

                @pl.when((link == at) & (step >= lag) & (step < chunks + lag))
                def _():
                    where = jnp.int32(to)
                    arrive(step - lag, where, to > at)
                    send(step - lag, where, to > at)

    def close(chunk):
        @pl.when(link > 0)
        def _():
            arrive(chunk, link, True)

        @pl.when(link < CHAIN - 1)
        def _():
            arrive(chunk, link, False)

        coeffs, variance = finish([part[chunk, link, k] for k in range(SUMS)])
        rows = pl.ds(pl.multiple_of(chunk * ROWS, ROWS), ROWS)
        for k in range(HARM):
            coeff_out[k, rows, :] = coeffs[k]
        var_out[rows, :] = variance

    lax.fori_loop(0, AHEAD, lambda step, _: (spread(step), 0)[1], 0)
    close_lag = by_link(CLOSE)

    def body(step, carry):
        spread(step + AHEAD)
        await_boxes(step)
        each(step, add_up)
        free_members(step)
        relay(step)

        @pl.when((step >= close_lag) & (step < chunks + close_lag))
        def _():
            close(step - close_lag)

        free_boxes(step)
        return carry

    lax.fori_loop(0, chunks + max(max(CLOSE), LAST_SENT), body, 0)

    lons = pl.ds(0, (members - 1) * CHAIN * LANES)
    sent = field.at[:, :, lons] if local_rows % lat == 0 else field.at[:, lons]
    pltpu.make_async_copy(sent, sent, raw_send).wait()
    passed = part.at[:, pl.ds(0, CHAIN - 1)]
    pltpu.make_async_copy(passed, passed, part_send).wait()


def put_out(coeffs, variance, coeff_out, var_out, sem):
    copies = [
        pltpu.make_async_copy(coeffs, coeff_out, sem.at[0]),
        pltpu.make_async_copy(variance, var_out, sem.at[1]),
    ]
    for copy in copies:
        copy.start()
    for copy in copies:
        copy.wait()


def local(snapshots):
    groups = lax.axis_size("io")
    local_rows, width = snapshots.shape
    lat = local_rows * groups // TIMES
    if width != groups * LANES or lat % ROWS or local_rows % ROWS or groups % CHAIN:
        raise ValueError("unsupported sizes")
    chunks = lat // ROWS
    members = groups // CHAIN
    field = snapshots.reshape(local_rows // lat, lat, width) if local_rows % lat == 0 else snapshots
    results = pl.pallas_call(
        functools.partial(kernel, groups, lat, local_rows),
        out_shape=(
            jax.ShapeDtypeStruct((HARM, lat, LANES), jnp.float32),
            jax.ShapeDtypeStruct((lat, LANES), jnp.float32),
        ),
        in_specs=[pl.BlockSpec(memory_space=pl.ANY)],
        out_specs=(pl.BlockSpec(memory_space=pltpu.VMEM), pl.BlockSpec(memory_space=pltpu.VMEM)),
        scratch_shapes=[
            pltpu.VMEM((chunks, CHAIN, SPAN, ROWS, LANES), jnp.float32),
            pltpu.VMEM((chunks, CHAIN, SUMS, ROWS, LANES), jnp.float32),
            pltpu.VMEM((chunks, CHAIN, SUMS, ROWS, LANES), jnp.float32),
            pltpu.VMEM((chunks, CHAIN, SUMS, ROWS, LANES), jnp.float32),
            pltpu.SemaphoreType.DMA,
            pltpu.SemaphoreType.DMA((RAW_SLOTS, CHAIN)),
            pltpu.SemaphoreType.DMA,
            pltpu.SemaphoreType.DMA((BOX_SLOTS, CHAIN + 1)),
            pltpu.SemaphoreType.REGULAR((members,)),
            pltpu.SemaphoreType.REGULAR((2,)),
        ],
        compiler_params=pltpu.CompilerParams(
            collective_id=0, has_side_effects=True, vmem_limit_bytes=44 * 2**20
        ),
        name="climatology",
    )(field)
    return pl.pallas_call(
        put_out,
        out_shape=tuple(jax.ShapeDtypeStruct(r.shape, r.dtype) for r in results),
        in_specs=[pl.BlockSpec(memory_space=pltpu.VMEM)] * 2,
        out_specs=(pl.BlockSpec(memory_space=pl.ANY),) * 2,
        scratch_shapes=[pltpu.SemaphoreType.DMA((2,))],
        compiler_params=pltpu.CompilerParams(vmem_limit_bytes=4 * 2**20),
        name="put_out",
    )(*results)


def solution(mesh):
    return jax.shard_map(
        local,
        mesh=mesh,
        in_specs=(P(("rep", "io"), None),),
        out_specs=(P("rep", None, "io"), P("rep", "io")),
        check_vma=False,
    )
```

```python
import functools

import jax
import jax.numpy as jnp
import numpy as np
from jax import lax
from jax.experimental import pallas as pl
from jax.experimental.pallas import tpu as pltpu
from jax.sharding import PartitionSpec as P

TIMES = 96
HARM = 16
MONTHS = 12
SPAN = 24
CHAIN = TIMES // SPAN
SLOW = 4
SUMS = MONTHS + SLOW + 1
LANES = 128
ROWS = 8
AHEAD = 4
SKEW = 3
EARLY_EVEN, EARLY_ODD = 2, 1
EARLY = max(EARLY_EVEN, EARLY_ODD)
FORWARD = 2
MESH = pl.DeviceIdType.MESH


def schedule():
    far = [[to for to in sorted(range(CHAIN), key=lambda to: -abs(to - at)) if to != at] for at in range(CHAIN)]
    orders = [blocks + [at] for at, blocks in enumerate(far)]
    added = []
    for at in range(CHAIN):
        lags = {}
        for to in far[at]:
            side = [other for other in far[at] if (other > at) == (to > at)]
            lags[to] = SKEW * side.index(to)
        lags[at] = SKEW + 1 if at in (0, CHAIN - 1) else SKEW * (CHAIN - 2)
        added.append(lags)
    up, down = {}, {}
    for to in range(CHAIN):
        for at in range(to + 1):
            up[at, to] = added[0][to] if at == 0 else max(added[at][to], up[at - 1, to] + 1)
        for at in range(CHAIN - 1, to - 1, -1):
            down[at, to] = added[at][to] if at == CHAIN - 1 else max(added[at][to], down[at + 1, to] + 1)
    close = [max(up[at, at], down[at, at]) for at in range(CHAIN)]
    for at in range(CHAIN):
        up[at, at] = down[at, at] = close[at]
    hold = max(
        [up[at + 1, to] - up[at, to] for at, to in up if at < to]
        + [down[at - 1, to] - down[at, to] for at, to in down if at > to]
    )
    last = max([lag for (at, to), lag in up.items() if at < to] + [lag for (at, to), lag in down.items() if at > to])
    return orders, added, up, down, close, hold, last


ORDERS, ADDED, UP, DOWN, CLOSE, HOLD, LAST_SENT = schedule()
LAST_ADDED = max(max(lags.values()) for lags in ADDED)
RAW_SLOTS = AHEAD + 2
BOX_SLOTS = HOLD + 3


def fit_constants():
    steps = np.arange(TIMES, dtype=np.float64)
    slow = np.stack(
        [
            (steps - (TIMES - 1) / 2.0) / (TIMES / 2.0),
            np.cos(2.0 * np.pi * steps / TIMES),
            np.sin(2.0 * np.pi * steps / TIMES),
            np.cos(4.0 * np.pi * steps / TIMES),
        ],
        axis=1,
    )
    month = np.arange(MONTHS, dtype=np.float64)
    angles = 2.0 * np.pi * month / MONTHS
    periodic = [np.cos(j * angles) for j in range(7)] + [np.sin(j * angles) for j in range(1, 6)]
    unmix = np.linalg.inv(np.stack(periodic, axis=1))
    years = TIMES // MONTHS
    cross = slow.reshape(years, MONTHS, SLOW).sum(axis=0)
    inner = np.linalg.inv(slow.T @ slow - cross.T @ cross / years)
    return slow, cross, inner, unmix, years


def dot(weights, values):
    total = None
    for weight, value in zip(weights, values):
        term = value * np.float32(weight)
        total = term if total is None else total + term
    return total


def finish(sums):
    _, cross, inner, unmix, years = fit_constants()
    by_month, moments, squares = sums[:MONTHS], sums[MONTHS : MONTHS + SLOW], sums[-1]
    reduced = [moments[k] - dot(cross[:, k] / years, by_month) for k in range(SLOW)]
    slow = [dot(inner[k], reduced) for k in range(SLOW)]
    level = [(by_month[m] - dot(cross[m], slow)) * np.float32(1.0 / years) for m in range(MONTHS)]
    explained = slow[0] * moments[0]
    for k in range(1, SLOW):
        explained = explained + slow[k] * moments[k]
    for m in range(MONTHS):
        explained = explained + level[m] * by_month[m]
    half = MONTHS // 2
    even = [level[0]] + [level[m] + level[MONTHS - m] for m in range(1, half)] + [level[half]]
    odd = [level[m] - level[MONTHS - m] for m in range(1, half)]
    cosines = [dot(unmix[j, : half + 1], even) for j in range(half + 1)]
    sines = [dot(unmix[half + j, 1:half], odd) for j in range(1, half)]
    coeffs = [cosines[0], slow[0]] + cosines[1:] + sines + slow[1:]
    return coeffs, (squares - explained) * np.float32(1.0 / TIMES)


def kernel(
    groups, lat, local_rows,
    field, coeff_out, var_out,
    raw, part, below, above,
    raw_send, raw_recv, part_send, box_recv, member_free, box_free,
    *direct,
):
    members = groups // CHAIN
    chunks = lat // ROWS
    held = local_rows // lat
    early = EARLY if direct else 0
    if direct:
        stage, first_stage, passing, early_raw, stage_sem, passing_recv, early_recv, early_send = direct
    me = lax.axis_index("io")
    link, member = me // members, lax.rem(me, members)
    device = lambda at, who: {"io": at * members + who}

    span = fit_constants()[0][:SPAN]
    at_end = (link == 0) | (link == CHAIN - 1)
    early_of = lambda who: EARLY_ODD + (EARLY_EVEN - EARLY_ODD) * (1 - lax.rem(who, 2))
    own_early = early_of(member)
    def by_link(values):
        return sum((link == at).astype(jnp.int32) * values[at] for at in range(CHAIN))

    inner = by_link([1, 0, CHAIN - 1, CHAIN - 2])

    def block_of(chunk, to):
        lons = pl.ds(pl.multiple_of(to * members * LANES, LANES), members * LANES)
        return field.at[:, pl.ds(chunk * ROWS, ROWS), lons]

    first_to = by_link([ORDERS[at][0] for at in range(CHAIN)])
    if direct:
        pltpu.make_async_copy(block_of(0, first_to), first_stage, stage_sem.at[0]).start()

        @pl.when(at_end)
        def _():
            for chunk in range(early):
                pltpu.make_async_copy(block_of(chunk, inner), stage.at[chunk], stage_sem.at[1 + chunk]).start()

    barrier = pltpu.get_barrier_semaphore()
    for step in range(1, members):
        other = lax.rem(member + step, members)
        pl.semaphore_signal(barrier, inc=1, device_id=device(link, other), device_id_type=MESH)

    @pl.when(link > 0)
    def _():
        pl.semaphore_signal(barrier, inc=1, device_id=device(link - 1, member), device_id_type=MESH)

    @pl.when(link < CHAIN - 1)
    def _():
        pl.semaphore_signal(barrier, inc=1, device_id=device(link + 1, member), device_id_type=MESH)

    ends = (link == 0).astype(jnp.int32) + (link == CHAIN - 1).astype(jnp.int32)
    pl.semaphore_wait(barrier, members + 1 - ends)

    def spread_one(chunk, to, step, row, count=held, time=None, staged=None):
        other = lax.rem(member + step, members)
        time = member * held if time is None else time
        lon = pl.multiple_of((to * members + other) * LANES, LANES)
        if count is None:
            src = field.at[pl.ds(row, ROWS), pl.ds(lon, LANES)]
            dst = raw.at[chunk, to, time]
        else:
            src = field.at[:, pl.ds(row, ROWS), pl.ds(lon, LANES)]
            if staged is not None and step > 0:
                src = staged.at[:, :, pl.ds(pl.multiple_of(other * LANES, LANES), LANES)]
            dst = raw.at[chunk, to, pl.ds(time, count)]
        arrived = raw_recv.at[lax.rem(jnp.int32(chunk), RAW_SLOTS), to]
        if step == 0:
            pltpu.make_async_copy(src, dst, arrived).start()
        else:
            pltpu.make_async_remote_copy(
                src_ref=src, dst_ref=dst, send_sem=raw_send, recv_sem=arrived,
                device_id=device(link, other), device_id_type=MESH,
            ).start()

    def spread_rows(*where):
        for step in list(range(1, members)) + [0]:
            spread_one(where[0], where[1], step, *where[2:])

    def spread_block(chunk, to):
        if local_rows % lat == 0:
            count = local_rows // lat
            spread_rows(chunk, to, pl.multiple_of(chunk * ROWS, ROWS), count, member * count)
        else:
            first = member * local_rows
            for extra in range(local_rows // lat + 2):
                time = first // lat + extra
                row = time * lat + chunk * ROWS - first

                @pl.when((row >= 0) & (row < local_rows))
                def _():
                    spread_rows(chunk, to, pl.multiple_of(row, ROWS), None, time)

    def each(step, act, staged_first=False, skip=0):
        for rank in range(CHAIN):
            lag = by_link([ADDED[at][ORDERS[at][rank]] for at in range(CHAIN)])

            to = by_link([ORDERS[at][rank] for at in range(CHAIN)])
            begin = lag + 1 if staged_first and rank == 0 else lag

            @pl.when((step >= begin) & (step < chunks + lag) & ((step >= lag + skip) | ~at_end | (to != inner)))
            def _():
                act(step - lag, to)

    spread_steps = chunks + LAST_ADDED

    def spread(step):
        @pl.when((step >= RAW_SLOTS) & (step < spread_steps))
        def _():
            for away in range(1, members):
                pl.semaphore_wait(member_free.at[away], 1)

        each(step, spread_block, staged_first=bool(direct), skip=early)

    def free_members(step):
        @pl.when(step + RAW_SLOTS < spread_steps)
        def _():
            for away in range(1, members):
                other = lax.rem(member + away, members)
                pl.semaphore_signal(
                    member_free.at[members - away], inc=1, device_id=device(link, other), device_id_type=MESH
                )

    send_steps, slack = chunks + LAST_SENT, BOX_SLOTS - HOLD

    def await_boxes(step):
        for up in (True, False):

            @pl.when((link < CHAIN - 1 if up else link > 0) & (step >= slack) & (step < send_steps))
            def _():
                pl.semaphore_wait(box_free.at[0 if up else 1], 1)

    def free_boxes(step):
        for up in (True, False):

            @pl.when((link > 0 if up else link < CHAIN - 1) & (step + slack < send_steps))
            def _():
                pl.semaphore_signal(
                    box_free.at[0 if up else 1], inc=1,
                    device_id=device(link - 1 if up else link + 1, member), device_id_type=MESH,
                )

    def box_sem(chunk, to, up, at):
        where = to if up else to + (to == at).astype(jnp.int32) * (CHAIN - to)
        return box_recv.at[lax.rem(chunk, BOX_SLOTS), where]

    def send(chunk, to, up):
        at = link + 1 if up else link - 1
        pltpu.make_async_remote_copy(
            src_ref=part.at[chunk, to],
            dst_ref=(below if up else above).at[chunk, to],
            send_sem=part_send,
            recv_sem=box_sem(chunk, to, up, at),
            device_id=device(at, member),
            device_id_type=MESH,
        ).start()

    def take(chunk, to, box):
        for k in range(SUMS):
            part[chunk, to, k] = part[chunk, to, k] + box[chunk, to, k]

    def wait_box(chunk, to, up):
        box = below if up else above
        pltpu.make_async_copy(box.at[chunk, to], box.at[chunk, to], box_sem(chunk, to, up, link)).wait()

    def arrive(chunk, to, up):
        wait_box(chunk, to, up)
        take(chunk, to, below if up else above)

    def arrive_own(chunk, up):
        if early:
            stands_in = (link == (1 if up else CHAIN - 2)) & (chunk < own_early)

            @pl.when(stands_in)
            def _():
                got = early_raw.at[chunk]
                pltpu.make_async_copy(got, got, early_recv.at[chunk]).wait()
                sum_span(lambda time: early_raw[chunk, time], inner, below if up else above, chunk, link)

            @pl.when(~stands_in)
            def _():
                wait_box(chunk, link, up)

        else:
            wait_box(chunk, link, up)
        take(chunk, link, below if up else above)

    def sum_span(value_at, source, result, chunk, to):
        offset = source.astype(jnp.float32) * np.float32(SPAN / (TIMES / 2.0))
        quarter = lambda at: (source == at).astype(jnp.float32)
        turn_cos, turn_sin = quarter(0) - quarter(2), quarter(1) - quarter(3)
        flip = quarter(0) - quarter(1) + quarter(2) - quarter(3)
        local = [None] * (SLOW + 1)
        whole = None
        for month in range(MONTHS):
            kept = None
            for time in range(month, SPAN, MONTHS):
                value = value_at(time)
                kept = value if kept is None else kept + value
                terms = [value * np.float32(span[time, k]) for k in range(SLOW)] + [value * value]
                local = [term if own is None else own + term for own, term in zip(local, terms)]
            result[chunk, to, month] = kept
            whole = kept if whole is None else whole + kept
        trend, cosine, sine, double, squares = local
        result[chunk, to, MONTHS] = trend + whole * offset
        result[chunk, to, MONTHS + 1] = cosine * turn_cos - sine * turn_sin
        result[chunk, to, MONTHS + 2] = cosine * turn_sin + sine * turn_cos
        result[chunk, to, MONTHS + 3] = double * flip
        result[chunk, to, MONTHS + 4] = squares

    def add_up(chunk, to):
        pltpu.make_async_copy(
            raw.at[chunk, to], raw.at[chunk, to], raw_recv.at[lax.rem(chunk, RAW_SLOTS), to]
        ).wait()
        sum_span(lambda time: raw[chunk, to, time], link, part, chunk, to)

        @pl.when((link == 0) & (to > 0))
        def _():
            send(chunk, to, True)

        @pl.when((link == CHAIN - 1) & (to < CHAIN - 1))
        def _():
            send(chunk, to, False)

    def relay(step):
        for at in range(1, CHAIN - 1):
            for to in range(CHAIN):
                if to == at:
                    continue
                lag = UP[at, to] if to > at else DOWN[at, to]

                @pl.when((link == at) & (step >= lag) & (step < chunks + lag))
                def _():
                    where = jnp.int32(to)
                    arrive(step - lag, where, to > at)
                    send(step - lag, where, to > at)

    def close(chunk):
        @pl.when(link > 0)
        def _():
            arrive_own(chunk, True)

        @pl.when(link < CHAIN - 1)
        def _():
            arrive_own(chunk, False)

        coeffs, variance = finish([part[chunk, link, k] for k in range(SUMS)])
        rows = pl.ds(pl.multiple_of(chunk * ROWS, ROWS), ROWS)
        for k in range(HARM):
            coeff_out[k, rows, :] = coeffs[k]
        var_out[rows, :] = variance

    def each_early(act):
        for chunk in range(early):
            for away in range(members):
                other = lax.rem(member + away, members)
                pl.when(chunk < early_of(other))(functools.partial(act, chunk, away, other))

    def send_early(chunk, away, other):
        own = early_raw.at[chunk, pl.ds(member * held, held)]
        pltpu.make_async_remote_copy(
            src_ref=stage.at[chunk, :, :, pl.ds(pl.multiple_of(other * LANES, LANES), LANES)],
            dst_ref=passing.at[chunk, away - 1] if away else own,
            send_sem=raw_send if away else early_send,
            recv_sem=(passing_recv if away else early_recv).at[chunk],
            device_id=device(inner, member),
            device_id_type=MESH,
        ).start()

    def forward_early(chunk, away, other):
        if away:
            pltpu.make_async_remote_copy(
                src_ref=passing.at[chunk, away - 1],
                dst_ref=early_raw.at[chunk, pl.ds(member * held, held)],
                send_sem=early_send,
                recv_sem=early_recv.at[chunk],
                device_id=device(link, other),
                device_id_type=MESH,
            ).start()

    def wait_passed(sem_of):
        for chunk in range(early):
            even, odd = chunk < EARLY_EVEN, chunk < EARLY_ODD
            for parity in range(2):
                pieces = members // 2 * (even + odd) - (odd if parity else even)

                @pl.when(lax.rem(member, 2) == parity)
                def _():
                    got = passing.at[chunk, pl.ds(0, pieces)]
                    pltpu.make_async_copy(got, got, sem_of(chunk)).wait()

    def forward():
        wait_passed(lambda chunk: passing_recv.at[chunk])
        each_early(forward_early)

    if direct:
        pltpu.make_async_copy(first_stage, first_stage, stage_sem.at[0]).wait()
        spread_rows(jnp.int32(0), first_to, 0, held, member * held, first_stage)

        @pl.when(at_end)
        def _():
            for chunk in range(early):
                pltpu.make_async_copy(stage.at[chunk], stage.at[chunk], stage_sem.at[1 + chunk]).wait()
            each_early(send_early)

    lax.fori_loop(0, AHEAD, lambda step, _: (spread(step), 0)[1], 0)
    if early:

        @pl.when(at_end)
        def _():
            for chunk in range(EARLY):
                for away in range(members):
                    other = lax.rem(member + away, members)
                    pl.when(chunk >= early_of(other))(functools.partial(spread_one, chunk, inner, away, chunk * ROWS))
    close_lag = by_link(CLOSE)

    def body(step, carry):
        spread(step + AHEAD)
        await_boxes(step)
        each(step, add_up, skip=own_early if early else 0)
        free_members(step)
        relay(step)
        if early:
            pl.when((step == FORWARD) & ~at_end)(forward)

        @pl.when((step >= close_lag) & (step < chunks + close_lag))
        def _():
            close(step - close_lag)

        free_boxes(step)
        return carry

    lax.fori_loop(0, chunks + max(max(CLOSE), LAST_SENT), body, 0)

    lons = pl.ds(0, (members - 1) * CHAIN * LANES)
    sent = field.at[:, :, lons] if local_rows % lat == 0 else field.at[:, lons]
    pltpu.make_async_copy(sent, sent, raw_send).wait()
    passed = part.at[pl.ds(early, chunks - early), pl.ds(0, CHAIN - 1)]
    pltpu.make_async_copy(passed, passed, part_send).wait()
    if early:
        passed = part.at[pl.ds(0, early), pl.ds(0, CHAIN - 2)]
        pltpu.make_async_copy(passed, passed, part_send).wait()

        @pl.when(at_end)
        def _():
            for chunk in range(early):

                @pl.when(chunk < own_early)
                def _():
                    own = early_raw.at[chunk, pl.ds(0, held)]
                    pltpu.make_async_copy(own, own, early_send).wait()

                @pl.when(chunk >= own_early)
                def _():
                    passed = part.at[chunk, 0]
                    pltpu.make_async_copy(passed, passed, part_send).wait()

        @pl.when(~at_end)
        def _():
            passed = part.at[pl.ds(0, early), 0]
            pltpu.make_async_copy(passed, passed, part_send).wait()
            wait_passed(lambda chunk: early_send)


def put_out(coeffs, variance, coeff_out, var_out, sem):
    copies = [
        pltpu.make_async_copy(coeffs, coeff_out, sem.at[0]),
        pltpu.make_async_copy(variance, var_out, sem.at[1]),
    ]
    for copy in copies:
        copy.start()
    for copy in copies:
        copy.wait()


def local(snapshots):
    groups = lax.axis_size("io")
    local_rows, width = snapshots.shape
    lat = local_rows * groups // TIMES
    if width != groups * LANES or lat % ROWS or local_rows % ROWS or groups % CHAIN:
        raise ValueError("unsupported sizes")
    chunks = lat // ROWS
    members = groups // CHAIN
    held, whole = local_rows // lat, local_rows % lat == 0
    field = snapshots.reshape(held, lat, width) if whole else snapshots
    direct = [
        pltpu.VMEM((EARLY, held, ROWS, members * LANES), jnp.float32),
        pltpu.VMEM((held, ROWS, members * LANES), jnp.float32),
        pltpu.VMEM((EARLY, members - 1, held, ROWS, LANES), jnp.float32),
        pltpu.VMEM((EARLY, SPAN, ROWS, LANES), jnp.float32),
        pltpu.SemaphoreType.DMA((1 + EARLY,)),
        pltpu.SemaphoreType.DMA((EARLY,)),
        pltpu.SemaphoreType.DMA((EARLY,)),
        pltpu.SemaphoreType.DMA,
    ]
    results = pl.pallas_call(
        functools.partial(kernel, groups, lat, local_rows),
        out_shape=(
            jax.ShapeDtypeStruct((HARM, lat, LANES), jnp.float32),
            jax.ShapeDtypeStruct((lat, LANES), jnp.float32),
        ),
        in_specs=[pl.BlockSpec(memory_space=pl.ANY)],
        out_specs=(pl.BlockSpec(memory_space=pltpu.VMEM), pl.BlockSpec(memory_space=pltpu.VMEM)),
        scratch_shapes=[
            pltpu.VMEM((chunks, CHAIN, SPAN, ROWS, LANES), jnp.float32),
            pltpu.VMEM((chunks, CHAIN, SUMS, ROWS, LANES), jnp.float32),
            pltpu.VMEM((chunks, CHAIN, SUMS, ROWS, LANES), jnp.float32),
            pltpu.VMEM((chunks, CHAIN, SUMS, ROWS, LANES), jnp.float32),
            pltpu.SemaphoreType.DMA,
            pltpu.SemaphoreType.DMA((RAW_SLOTS, CHAIN)),
            pltpu.SemaphoreType.DMA,
            pltpu.SemaphoreType.DMA((BOX_SLOTS, CHAIN + 1)),
            pltpu.SemaphoreType.REGULAR((members,)),
            pltpu.SemaphoreType.REGULAR((2,)),
            *(direct if whole else []),
        ],
        compiler_params=pltpu.CompilerParams(
            collective_id=0, has_side_effects=True, vmem_limit_bytes=44 * 2**20
        ),
        name="climatology",
    )(field)
    return pl.pallas_call(
        put_out,
        out_shape=tuple(jax.ShapeDtypeStruct(r.shape, r.dtype) for r in results),
        in_specs=[pl.BlockSpec(memory_space=pltpu.VMEM)] * 2,
        out_specs=(pl.BlockSpec(memory_space=pl.ANY),) * 2,
        scratch_shapes=[pltpu.SemaphoreType.DMA((2,))],
        compiler_params=pltpu.CompilerParams(vmem_limit_bytes=4 * 2**20),
        name="put_out",
    )(*results)


def solution(mesh):
    return jax.shard_map(
        local,
        mesh=mesh,
        in_specs=(P(("rep", "io"), None),),
        out_specs=(P("rep", None, "io"), P("rep", "io")),
        check_vma=False,
    )
```

```python
import functools

import jax
import jax.numpy as jnp
import numpy as np
from jax import lax
from jax.experimental import pallas as pl
from jax.experimental.pallas import tpu as pltpu
from jax.sharding import PartitionSpec as P

TIMES = 96
HARM = 16
MONTHS = 12
SPAN = 24
CHAIN = TIMES // SPAN
SLOW = 4
SUMS = MONTHS + SLOW + 1
LANES = 128
ROWS = 8
AHEAD = 4
SKEW = 3
EARLY_EVEN, EARLY_ODD = 2, 1
EARLY = max(EARLY_EVEN, EARLY_ODD)
FORWARD = 2
MESH = pl.DeviceIdType.MESH


def schedule():
    orders, added = [], []
    for at in range(CHAIN):
        far = sorted((to for to in range(CHAIN) if to != at), key=lambda to: -abs(to - at))
        lags = {at: SKEW * (CHAIN - 2)}
        for to in far:
            side = [other for other in far if (other > at) == (to > at)]
            lags[to] = SKEW * side.index(to)
        orders.append(far + [at])
        added.append(lags)
    passed, close = {}, []
    for to in range(CHAIN):
        for way in (range(to + 1), range(CHAIN - 1, to - 1, -1)):
            lag = -1
            for at in way:
                lag = max(added[at][to], lag + 1)
                passed[at, to] = max(lag, passed.get((at, to), 0))
        close.append(passed[to, to])
    return orders, added, passed, close


ORDERS, ADDED, PASSED, CLOSE = schedule()


def fit_constants():
    steps = np.arange(TIMES, dtype=np.float64)
    slow = np.stack(
        [
            (steps - (TIMES - 1) / 2.0) / (TIMES / 2.0),
            np.cos(2.0 * np.pi * steps / TIMES),
            np.sin(2.0 * np.pi * steps / TIMES),
            np.cos(4.0 * np.pi * steps / TIMES),
        ],
        axis=1,
    )
    month = np.arange(MONTHS, dtype=np.float64)
    angles = 2.0 * np.pi * month / MONTHS
    periodic = [np.cos(j * angles) for j in range(7)] + [np.sin(j * angles) for j in range(1, 6)]
    unmix = np.linalg.inv(np.stack(periodic, axis=1))
    years = TIMES // MONTHS
    cross = slow.reshape(years, MONTHS, SLOW).sum(axis=0)
    inner = np.linalg.inv(slow.T @ slow - cross.T @ cross / years)
    return slow, cross, inner, unmix, years


def dot(weights, values):
    total = None
    for weight, value in zip(weights, values):
        term = value * np.float32(weight)
        total = term if total is None else total + term
    return total


def finish(sums):
    _, cross, inner, unmix, years = fit_constants()
    by_month, moments, squares = sums[:MONTHS], sums[MONTHS : MONTHS + SLOW], sums[-1]
    reduced = [moments[k] - dot(cross[:, k] / years, by_month) for k in range(SLOW)]
    slow = [dot(inner[k], reduced) for k in range(SLOW)]
    level = [(by_month[m] - dot(cross[m], slow)) * np.float32(1.0 / years) for m in range(MONTHS)]
    explained = slow[0] * moments[0]
    for k in range(1, SLOW):
        explained = explained + slow[k] * moments[k]
    for m in range(MONTHS):
        explained = explained + level[m] * by_month[m]
    half = MONTHS // 2
    even = [level[0]] + [level[m] + level[MONTHS - m] for m in range(1, half)] + [level[half]]
    odd = [level[m] - level[MONTHS - m] for m in range(1, half)]
    cosines = [dot(unmix[j, : half + 1], even) for j in range(half + 1)]
    sines = [dot(unmix[half + j, 1:half], odd) for j in range(1, half)]
    coeffs = [cosines[0], slow[0]] + cosines[1:] + sines + slow[1:]
    return coeffs, (squares - explained) * np.float32(1.0 / TIMES)


def kernel(
    groups, lat, local_rows,
    field, coeff_out, var_out,
    raw, part, below, above, direct,
    raw_send, raw_recv, part_send, box_recv, *direct_sems,
):
    members = groups // CHAIN
    chunks = lat // ROWS
    held = local_rows // lat
    early = EARLY if direct else 0
    if direct:
        stage, first_stage, passing, early_raw = direct
        stage_sem, passing_recv, early_recv, early_send = direct_sems
    me = lax.axis_index("io")
    link, member = me // members, lax.rem(me, members)
    device = lambda at, who: {"io": at * members + who}

    span = fit_constants()[0][:SPAN]
    at_end = (link == 0) | (link == CHAIN - 1)
    early_of = lambda who: EARLY_ODD + (EARLY_EVEN - EARLY_ODD) * (1 - lax.rem(who, 2))
    own_early = early_of(member)
    def by_link(values):
        return sum((link == at).astype(jnp.int32) * values[at] for at in range(CHAIN))

    inner = by_link([1, 0, CHAIN - 1, CHAIN - 2])

    def block_of(chunk, to):
        lons = pl.ds(pl.multiple_of(to * members * LANES, LANES), members * LANES)
        return field.at[:, pl.ds(chunk * ROWS, ROWS), lons]

    barrier = pltpu.get_barrier_semaphore()
    @pl.when(link > 0)
    def _():
        pl.semaphore_signal(barrier, inc=1, device_id=device(link - 1, member), device_id_type=MESH)

    @pl.when(link < CHAIN - 1)
    def _():
        pl.semaphore_signal(barrier, inc=1, device_id=device(link + 1, member), device_id_type=MESH)

    for step in range(1, members):
        other = lax.rem(member + step, members)
        pl.semaphore_signal(barrier, inc=1, device_id=device(link, other), device_id_type=MESH)

    first_to = by_link([ORDERS[at][0] for at in range(CHAIN)])
    if direct:
        pltpu.make_async_copy(block_of(0, first_to), first_stage, stage_sem.at[0]).start()

        @pl.when(at_end)
        def _():
            for chunk in range(early):
                pltpu.make_async_copy(block_of(chunk, inner), stage.at[chunk], stage_sem.at[1 + chunk]).start()

    ends = (link == 0).astype(jnp.int32) + (link == CHAIN - 1).astype(jnp.int32)
    pl.semaphore_wait(barrier, members + 1 - ends)

    def spread_one(chunk, to, step, row, count=held, time=None, staged=None):
        other = lax.rem(member + step, members)
        time = member * held if time is None else time
        lon = pl.multiple_of((to * members + other) * LANES, LANES)
        if count is None:
            src = field.at[pl.ds(row, ROWS), pl.ds(lon, LANES)]
            dst = raw.at[chunk, to, time]
        else:
            src = field.at[:, pl.ds(row, ROWS), pl.ds(lon, LANES)]
            if staged is not None and step > 0:
                src = staged.at[:, :, pl.ds(pl.multiple_of(other * LANES, LANES), LANES)]
            dst = raw.at[chunk, to, pl.ds(time, count)]
        arrived = raw_recv.at[chunk, to]
        if step == 0:
            pltpu.make_async_copy(src, dst, arrived).start()
        else:
            pltpu.make_async_remote_copy(
                src_ref=src, dst_ref=dst, send_sem=raw_send, recv_sem=arrived,
                device_id=device(link, other), device_id_type=MESH,
            ).start()

    def spread_rows(*where):
        for step in list(range(1, members)) + [0]:
            spread_one(where[0], where[1], step, *where[2:])

    def spread_block(chunk, to):
        if local_rows % lat == 0:
            count = local_rows // lat
            spread_rows(chunk, to, pl.multiple_of(chunk * ROWS, ROWS), count, member * count)
        else:
            first = member * local_rows
            for extra in range(local_rows // lat + 2):
                time = first // lat + extra
                row = time * lat + chunk * ROWS - first

                @pl.when((row >= 0) & (row < local_rows))
                def _():
                    spread_rows(chunk, to, pl.multiple_of(row, ROWS), None, time)

    def each(step, act, staged_first=False, skip=0):
        for rank in range(CHAIN):
            lag = by_link([ADDED[at][ORDERS[at][rank]] for at in range(CHAIN)])

            to = by_link([ORDERS[at][rank] for at in range(CHAIN)])
            begin = lag + 1 if staged_first and rank == 0 else lag

            @pl.when((step >= begin) & (step < chunks + lag) & ((step >= lag + skip) | ~at_end | (to != inner)))
            def _():
                act(step - lag, to)

    def spread(step):
        each(step, spread_block, staged_first=bool(direct), skip=early)

    def box_sem(chunk, to, up, at):
        where = to if up else to + (to == at).astype(jnp.int32) * (CHAIN - to)
        return box_recv.at[chunk, where]

    def send(chunk, to, up):
        at = link + 1 if up else link - 1
        pltpu.make_async_remote_copy(
            src_ref=part.at[chunk, to],
            dst_ref=(below if up else above).at[chunk, to],
            send_sem=part_send,
            recv_sem=box_sem(chunk, to, up, at),
            device_id=device(at, member),
            device_id_type=MESH,
        ).start()

    def take(chunk, to, box):
        for k in range(SUMS):
            part[chunk, to, k] = part[chunk, to, k] + box[chunk, to, k]

    def wait_box(chunk, to, up):
        box = below if up else above
        pltpu.make_async_copy(box.at[chunk, to], box.at[chunk, to], box_sem(chunk, to, up, link)).wait()

    def arrive(chunk, to, up):
        wait_box(chunk, to, up)
        take(chunk, to, below if up else above)

    def arrive_own(chunk, up):
        if early:
            stands_in = (link == (1 if up else CHAIN - 2)) & (chunk < own_early)

            @pl.when(stands_in)
            def _():
                got = early_raw.at[chunk]
                pltpu.make_async_copy(got, got, early_recv.at[chunk]).wait()
                sum_span(lambda time: early_raw[chunk, time], inner, below if up else above, chunk, link)

            @pl.when(~stands_in)
            def _():
                wait_box(chunk, link, up)

        else:
            wait_box(chunk, link, up)
        take(chunk, link, below if up else above)

    def sum_span(value_at, source, result, chunk, to):
        offset = source.astype(jnp.float32) * np.float32(SPAN / (TIMES / 2.0))
        quarter = lambda at: (source == at).astype(jnp.float32)
        turn_cos, turn_sin = quarter(0) - quarter(2), quarter(1) - quarter(3)
        flip = quarter(0) - quarter(1) + quarter(2) - quarter(3)
        local = [None] * (SLOW + 1)
        whole = None
        for month in range(MONTHS):
            kept = None
            for time in range(month, SPAN, MONTHS):
                value = value_at(time)
                kept = value if kept is None else kept + value
                terms = [value * np.float32(span[time, k]) for k in range(SLOW)] + [value * value]
                local = [term if own is None else own + term for own, term in zip(local, terms)]
            result[chunk, to, month] = kept
            whole = kept if whole is None else whole + kept
        trend, cosine, sine, double, squares = local
        result[chunk, to, MONTHS] = trend + whole * offset
        result[chunk, to, MONTHS + 1] = cosine * turn_cos - sine * turn_sin
        result[chunk, to, MONTHS + 2] = cosine * turn_sin + sine * turn_cos
        result[chunk, to, MONTHS + 3] = double * flip
        result[chunk, to, MONTHS + 4] = squares

    def add_up(chunk, to):
        pltpu.make_async_copy(
            raw.at[chunk, to], raw.at[chunk, to], raw_recv.at[chunk, to]
        ).wait()
        sum_span(lambda time: raw[chunk, to, time], link, part, chunk, to)

        @pl.when((link == 0) & (to > 0))
        def _():
            send(chunk, to, True)

        @pl.when((link == CHAIN - 1) & (to < CHAIN - 1))
        def _():
            send(chunk, to, False)

    def relay(step):
        for at in range(1, CHAIN - 1):
            for to in range(CHAIN):
                if to == at:
                    continue
                lag = PASSED[at, to]

                @pl.when((link == at) & (step >= lag) & (step < chunks + lag))
                def _():
                    where = jnp.int32(to)
                    arrive(step - lag, where, to > at)
                    send(step - lag, where, to > at)

    def close(chunk):
        @pl.when(link > 0)
        def _():
            arrive_own(chunk, True)

        @pl.when(link < CHAIN - 1)
        def _():
            arrive_own(chunk, False)

        coeffs, variance = finish([part[chunk, link, k] for k in range(SUMS)])
        rows = pl.ds(pl.multiple_of(chunk * ROWS, ROWS), ROWS)
        for k in range(HARM):
            coeff_out[k, rows, :] = coeffs[k]
        var_out[rows, :] = variance

    def each_early(act):
        for chunk in range(early):
            for away in range(members):
                other = lax.rem(member + away, members)
                pl.when(chunk < early_of(other))(functools.partial(act, chunk, away, other))

    def send_early(chunk, away, other):
        own = early_raw.at[chunk, pl.ds(member * held, held)]
        pltpu.make_async_remote_copy(
            src_ref=stage.at[chunk, :, :, pl.ds(pl.multiple_of(other * LANES, LANES), LANES)],
            dst_ref=passing.at[chunk, away - 1] if away else own,
            send_sem=raw_send if away else early_send,
            recv_sem=(passing_recv if away else early_recv).at[chunk],
            device_id=device(inner, member),
            device_id_type=MESH,
        ).start()

    def forward_early(chunk, away, other):
        if away:
            pltpu.make_async_remote_copy(
                src_ref=passing.at[chunk, away - 1],
                dst_ref=early_raw.at[chunk, pl.ds(member * held, held)],
                send_sem=early_send,
                recv_sem=early_recv.at[chunk],
                device_id=device(link, other),
                device_id_type=MESH,
            ).start()

    def wait_passed(sem_of):
        for chunk in range(early):
            even, odd = chunk < EARLY_EVEN, chunk < EARLY_ODD
            for parity in range(2):
                pieces = members // 2 * (even + odd) - (odd if parity else even)

                @pl.when(lax.rem(member, 2) == parity)
                def _():
                    got = passing.at[chunk, pl.ds(0, pieces)]
                    pltpu.make_async_copy(got, got, sem_of(chunk)).wait()

    def forward():
        wait_passed(lambda chunk: passing_recv.at[chunk])
        each_early(forward_early)

    if direct:
        pltpu.make_async_copy(first_stage, first_stage, stage_sem.at[0]).wait()
        spread_rows(jnp.int32(0), first_to, 0, held, member * held, first_stage)

        @pl.when(at_end)
        def _():
            for chunk in range(early):
                pltpu.make_async_copy(stage.at[chunk], stage.at[chunk], stage_sem.at[1 + chunk]).wait()
            each_early(send_early)

    lax.fori_loop(0, AHEAD, lambda step, _: (spread(step), 0)[1], 0)
    if early:

        @pl.when(at_end)
        def _():
            for chunk in range(EARLY):
                for away in range(members):
                    other = lax.rem(member + away, members)
                    pl.when(chunk >= early_of(other))(functools.partial(spread_one, chunk, inner, away, chunk * ROWS))
    close_lag = by_link(CLOSE)

    def body(step, carry):
        spread(step + AHEAD)
        each(step, add_up, skip=own_early if early else 0)
        relay(step)
        if early:
            pl.when((step == FORWARD) & ~at_end)(forward)

        @pl.when((step >= close_lag) & (step < chunks + close_lag))
        def _():
            close(step - close_lag)

        return carry

    lax.fori_loop(0, chunks + max(PASSED.values()), body, 0)

    lons = pl.ds(0, (members - 1) * CHAIN * LANES)
    sent = field.at[:, :, lons] if local_rows % lat == 0 else field.at[:, lons]
    pltpu.make_async_copy(sent, sent, raw_send).wait()
    passed = part.at[pl.ds(early, chunks - early), pl.ds(0, CHAIN - 1)]
    pltpu.make_async_copy(passed, passed, part_send).wait()
    if early:
        passed = part.at[pl.ds(0, early), pl.ds(0, CHAIN - 2)]
        pltpu.make_async_copy(passed, passed, part_send).wait()

        @pl.when(at_end)
        def _():
            for chunk in range(early):

                @pl.when(chunk < own_early)
                def _():
                    own = early_raw.at[chunk, pl.ds(0, held)]
                    pltpu.make_async_copy(own, own, early_send).wait()

                @pl.when(chunk >= own_early)
                def _():
                    passed = part.at[chunk, 0]
                    pltpu.make_async_copy(passed, passed, part_send).wait()

        @pl.when(~at_end)
        def _():
            passed = part.at[pl.ds(0, early), 0]
            pltpu.make_async_copy(passed, passed, part_send).wait()
            wait_passed(lambda chunk: early_send)


def scoped(groups, lat, local_rows, field, coeff_out, var_out, raw, part, below, above, *direct):
    chunks = lat // ROWS
    sems = [
        pltpu.SemaphoreType.DMA,
        pltpu.SemaphoreType.DMA((chunks, CHAIN)),
        pltpu.SemaphoreType.DMA,
        pltpu.SemaphoreType.DMA((chunks, CHAIN + 1)),
    ]
    if direct:
        sems += [
            pltpu.SemaphoreType.DMA((1 + EARLY,)),
            pltpu.SemaphoreType.DMA((EARLY,)),
            pltpu.SemaphoreType.DMA((EARLY,)),
            pltpu.SemaphoreType.DMA,
        ]
    pl.run_scoped(
        functools.partial(
            kernel, groups, lat, local_rows, field, coeff_out, var_out, raw, part, below, above, direct
        ),
        *sems,
    )


def put_out(coeffs, variance, coeff_out, var_out, sem):
    copies = [
        pltpu.make_async_copy(coeffs, coeff_out, sem.at[0]),
        pltpu.make_async_copy(variance, var_out, sem.at[1]),
    ]
    for copy in copies:
        copy.start()
    for copy in copies:
        copy.wait()


def local(snapshots):
    groups = lax.axis_size("io")
    local_rows, width = snapshots.shape
    lat = local_rows * groups // TIMES
    if width != groups * LANES or lat % ROWS or local_rows % ROWS or groups % CHAIN:
        raise ValueError("unsupported sizes")
    chunks = lat // ROWS
    members = groups // CHAIN
    held, whole = local_rows // lat, local_rows % lat == 0
    field = snapshots.reshape(held, lat, width) if whole else snapshots
    direct = [
        pltpu.VMEM((EARLY, held, ROWS, members * LANES), jnp.float32),
        pltpu.VMEM((held, ROWS, members * LANES), jnp.float32),
        pltpu.VMEM((EARLY, members - 1, held, ROWS, LANES), jnp.float32),
        pltpu.VMEM((EARLY, SPAN, ROWS, LANES), jnp.float32),
    ]
    results = pl.pallas_call(
        functools.partial(scoped, groups, lat, local_rows),
        out_shape=(
            jax.ShapeDtypeStruct((HARM, lat, LANES), jnp.float32),
            jax.ShapeDtypeStruct((lat, LANES), jnp.float32),
        ),
        in_specs=[pl.BlockSpec(memory_space=pl.ANY)],
        out_specs=(pl.BlockSpec(memory_space=pltpu.VMEM), pl.BlockSpec(memory_space=pltpu.VMEM)),
        scratch_shapes=[
            pltpu.VMEM((chunks, CHAIN, SPAN, ROWS, LANES), jnp.float32),
            pltpu.VMEM((chunks, CHAIN, SUMS, ROWS, LANES), jnp.float32),
            pltpu.VMEM((chunks, CHAIN, SUMS, ROWS, LANES), jnp.float32),
            pltpu.VMEM((chunks, CHAIN, SUMS, ROWS, LANES), jnp.float32),
            *(direct if whole else []),
        ],
        compiler_params=pltpu.CompilerParams(
            collective_id=0, has_side_effects=True, vmem_limit_bytes=44 * 2**20
        ),
        name="climatology",
    )(field)
    return pl.pallas_call(
        put_out,
        out_shape=tuple(jax.ShapeDtypeStruct(r.shape, r.dtype) for r in results),
        in_specs=[pl.BlockSpec(memory_space=pltpu.VMEM)] * 2,
        out_specs=(pl.BlockSpec(memory_space=pl.ANY),) * 2,
        scratch_shapes=[pltpu.SemaphoreType.DMA((2,))],
        compiler_params=pltpu.CompilerParams(vmem_limit_bytes=4 * 2**20),
        name="put_out",
    )(*results)


def solution(mesh):
    return jax.shard_map(
        local,
        mesh=mesh,
        in_specs=(P(("rep", "io"), None),),
        out_specs=(P("rep", None, "io"), P("rep", "io")),
        check_vma=False,
    )
```

```python
import functools

import jax
import jax.numpy as jnp
import numpy as np
from jax import lax
from jax.experimental import pallas as pl
from jax.experimental.pallas import tpu as pltpu
from jax.sharding import PartitionSpec as P

TIMES = 96
HARM = 16
MONTHS = 12
SPAN = 24
CHAIN = TIMES // SPAN
SLOW = 4
SUMS = MONTHS + SLOW + 1
LANES = 128
ROWS = 8
AHEAD = 4
SKEW = 3
EARLY_EVEN, EARLY_ODD = 2, 1
EARLY = max(EARLY_EVEN, EARLY_ODD)
FORWARD = 2
MESH = pl.DeviceIdType.MESH


def schedule():
    orders, added = [], []
    for at in range(CHAIN):
        far = sorted((to for to in range(CHAIN) if to != at), key=lambda to: -abs(to - at))
        lags = {at: SKEW * (CHAIN - 2)}
        for to in far:
            side = [other for other in far if (other > at) == (to > at)]
            lags[to] = SKEW * side.index(to)
        orders.append(far + [at])
        added.append(lags)
    passed, close = {}, []
    for to in range(CHAIN):
        for way in (range(to + 1), range(CHAIN - 1, to - 1, -1)):
            lag = -1
            for at in way:
                lag = max(added[at][to], lag + 1)
                passed[at, to] = max(lag, passed.get((at, to), 0))
        close.append(passed[to, to])
    return orders, added, passed, close


ORDERS, ADDED, PASSED, CLOSE = schedule()


def fit_constants():
    steps = np.arange(TIMES, dtype=np.float64)
    slow = np.stack(
        [
            (steps - (TIMES - 1) / 2.0) / (TIMES / 2.0),
            np.cos(2.0 * np.pi * steps / TIMES),
            np.sin(2.0 * np.pi * steps / TIMES),
            np.cos(4.0 * np.pi * steps / TIMES),
        ],
        axis=1,
    )
    month = np.arange(MONTHS, dtype=np.float64)
    angles = 2.0 * np.pi * month / MONTHS
    periodic = [np.cos(j * angles) for j in range(7)] + [np.sin(j * angles) for j in range(1, 6)]
    unmix = np.linalg.inv(np.stack(periodic, axis=1))
    years = TIMES // MONTHS
    cross = slow.reshape(years, MONTHS, SLOW).sum(axis=0)
    inner = np.linalg.inv(slow.T @ slow - cross.T @ cross / years)
    return slow, cross, inner, unmix, years


def dot(weights, values):
    total = None
    for weight, value in zip(weights, values):
        term = value * np.float32(weight)
        total = term if total is None else total + term
    return total


def finish(sums):
    _, cross, inner, unmix, years = fit_constants()
    by_month, moments, squares = sums[:MONTHS], sums[MONTHS : MONTHS + SLOW], sums[-1]
    reduced = [moments[k] - dot(cross[:, k] / years, by_month) for k in range(SLOW)]
    slow = [dot(inner[k], reduced) for k in range(SLOW)]
    level = [(by_month[m] - dot(cross[m], slow)) * np.float32(1.0 / years) for m in range(MONTHS)]
    explained = slow[0] * moments[0]
    for k in range(1, SLOW):
        explained = explained + slow[k] * moments[k]
    for m in range(MONTHS):
        explained = explained + level[m] * by_month[m]
    half = MONTHS // 2
    even = [level[0]] + [level[m] + level[MONTHS - m] for m in range(1, half)] + [level[half]]
    odd = [level[m] - level[MONTHS - m] for m in range(1, half)]
    cosines = [dot(unmix[j, : half + 1], even) for j in range(half + 1)]
    sines = [dot(unmix[half + j, 1:half], odd) for j in range(1, half)]
    coeffs = [cosines[0], slow[0]] + cosines[1:] + sines + slow[1:]
    return coeffs, (squares - explained) * np.float32(1.0 / TIMES)


def kernel(
    groups, lat, local_rows,
    field, coeff_out, var_out,
    raw, part, below, above, direct,
    raw_send, raw_recv, part_send, box_recv, *direct_sems,
):
    members = groups // CHAIN
    chunks = lat // ROWS
    held = local_rows // lat
    early = EARLY if direct else 0
    if direct:
        stage, first_stage, passing, early_raw = direct
        stage_sem, passing_recv, early_recv, early_send = direct_sems
    me = lax.axis_index("io")
    link, member = me // members, lax.rem(me, members)
    device = lambda at, who: {"io": at * members + who}

    span = fit_constants()[0][:SPAN]
    at_end = (link == 0) | (link == CHAIN - 1)
    early_of = lambda who: EARLY_ODD + (EARLY_EVEN - EARLY_ODD) * (1 - lax.rem(who, 2))
    own_early = early_of(member)
    def by_link(values):
        return sum((link == at).astype(jnp.int32) * values[at] for at in range(CHAIN))

    inner = by_link([1, 0, CHAIN - 1, CHAIN - 2])

    def block_of(chunk, to):
        lons = pl.ds(pl.multiple_of(to * members * LANES, LANES), members * LANES)
        return field.at[:, pl.ds(chunk * ROWS, ROWS), lons]

    barrier = pltpu.get_barrier_semaphore()
    @pl.when(link > 0)
    def _():
        pl.semaphore_signal(barrier, inc=1, device_id=device(link - 1, member), device_id_type=MESH)

    @pl.when(link < CHAIN - 1)
    def _():
        pl.semaphore_signal(barrier, inc=1, device_id=device(link + 1, member), device_id_type=MESH)

    for step in range(1, members):
        other = lax.rem(member + step, members)
        pl.semaphore_signal(barrier, inc=1, device_id=device(link, other), device_id_type=MESH)

    first_to = by_link([ORDERS[at][0] for at in range(CHAIN)])
    if direct:
        pltpu.make_async_copy(block_of(0, first_to), first_stage, stage_sem.at[0]).start()

        @pl.when(at_end)
        def _():
            for chunk in range(early):
                pltpu.make_async_copy(block_of(chunk, inner), stage.at[chunk], stage_sem.at[1 + chunk]).start()

    ends = (link == 0).astype(jnp.int32) + (link == CHAIN - 1).astype(jnp.int32)
    pl.semaphore_wait(barrier, members + 1 - ends)

    def spread_one(chunk, to, step, row, count=held, time=None, staged=None):
        other = lax.rem(member + step, members)
        time = member * held if time is None else time
        lon = pl.multiple_of((to * members + other) * LANES, LANES)
        if count is None:
            src = field.at[pl.ds(row, ROWS), pl.ds(lon, LANES)]
            dst = raw.at[chunk, to, time]
        else:
            src = field.at[:, pl.ds(row, ROWS), pl.ds(lon, LANES)]
            if staged is not None and step > 0:
                src = staged.at[:, :, pl.ds(pl.multiple_of(other * LANES, LANES), LANES)]
            dst = raw.at[chunk, to, pl.ds(time, count)]
        arrived = raw_recv.at[chunk, to]
        if step == 0:
            pltpu.make_async_copy(src, dst, arrived).start()
        else:
            pltpu.make_async_remote_copy(
                src_ref=src, dst_ref=dst, send_sem=raw_send, recv_sem=arrived,
                device_id=device(link, other), device_id_type=MESH,
            ).start()

    def spread_rows(*where):
        for step in list(range(1, members)) + [0]:
            spread_one(where[0], where[1], step, *where[2:])

    def spread_block(chunk, to):
        if local_rows % lat == 0:
            count = local_rows // lat
            spread_rows(chunk, to, pl.multiple_of(chunk * ROWS, ROWS), count, member * count)
        else:
            first = member * local_rows
            for extra in range(local_rows // lat + 2):
                time = first // lat + extra
                row = time * lat + chunk * ROWS - first

                @pl.when((row >= 0) & (row < local_rows))
                def _():
                    spread_rows(chunk, to, pl.multiple_of(row, ROWS), None, time)

    def each(step, act, staged_first=False, skip=0):
        for rank in range(CHAIN):
            lag = by_link([ADDED[at][ORDERS[at][rank]] for at in range(CHAIN)])

            to = by_link([ORDERS[at][rank] for at in range(CHAIN)])
            begin = lag + 1 if staged_first and rank == 0 else lag

            @pl.when((step >= begin) & (step < chunks + lag) & ((step >= lag + skip) | ~at_end | (to != inner)))
            def _():
                act(step - lag, to)

    def spread(step):
        each(step, spread_block, staged_first=bool(direct), skip=early)

    def box_sem(chunk, to, up, at):
        where = to if up else to + (to == at).astype(jnp.int32) * (CHAIN - to)
        return box_recv.at[chunk, where]

    def send(chunk, to, up):
        at = link + 1 if up else link - 1
        pltpu.make_async_remote_copy(
            src_ref=part.at[chunk, to],
            dst_ref=(below if up else above).at[chunk, to],
            send_sem=part_send,
            recv_sem=box_sem(chunk, to, up, at),
            device_id=device(at, member),
            device_id_type=MESH,
        ).start()

    def take(chunk, to, box):
        for k in range(SUMS):
            part[chunk, to, k] = part[chunk, to, k] + box[chunk, to, k]

    def wait_box(chunk, to, up):
        box = below if up else above
        pltpu.make_async_copy(box.at[chunk, to], box.at[chunk, to], box_sem(chunk, to, up, link)).wait()

    def arrive(chunk, to, up):
        wait_box(chunk, to, up)
        take(chunk, to, below if up else above)

    def arrive_own(chunk, up):
        if early:
            stands_in = (link == (1 if up else CHAIN - 2)) & (chunk < own_early)

            @pl.when(stands_in)
            def _():
                got = early_raw.at[chunk]
                pltpu.make_async_copy(got, got, early_recv.at[chunk]).wait()
                sum_span(lambda time: early_raw[chunk, time], inner, below if up else above, chunk, link)

            @pl.when(~stands_in)
            def _():
                wait_box(chunk, link, up)

        else:
            wait_box(chunk, link, up)
        take(chunk, link, below if up else above)

    def sum_span(value_at, source, result, chunk, to):
        offset = source.astype(jnp.float32) * np.float32(SPAN / (TIMES / 2.0))
        quarter = lambda at: (source == at).astype(jnp.float32)
        turn_cos, turn_sin = quarter(0) - quarter(2), quarter(1) - quarter(3)
        flip = quarter(0) - quarter(1) + quarter(2) - quarter(3)
        local = [None] * (SLOW + 1)
        whole = None
        for month in range(MONTHS):
            kept = None
            for time in range(month, SPAN, MONTHS):
                value = value_at(time)
                kept = value if kept is None else kept + value
                terms = [value * np.float32(span[time, k]) for k in range(SLOW)] + [value * value]
                local = [term if own is None else own + term for own, term in zip(local, terms)]
            result[chunk, to, month] = kept
            whole = kept if whole is None else whole + kept
        trend, cosine, sine, double, squares = local
        result[chunk, to, MONTHS] = trend + whole * offset
        result[chunk, to, MONTHS + 1] = cosine * turn_cos - sine * turn_sin
        result[chunk, to, MONTHS + 2] = cosine * turn_sin + sine * turn_cos
        result[chunk, to, MONTHS + 3] = double * flip
        result[chunk, to, MONTHS + 4] = squares

    def add_up(chunk, to):
        pltpu.make_async_copy(
            raw.at[chunk, to], raw.at[chunk, to], raw_recv.at[chunk, to]
        ).wait()
        sum_span(lambda time: raw[chunk, to, time], link, part, chunk, to)

        @pl.when((link == 0) & (to > 0))
        def _():
            send(chunk, to, True)

        @pl.when((link == CHAIN - 1) & (to < CHAIN - 1))
        def _():
            send(chunk, to, False)

    def relay(step):
        for at in range(1, CHAIN - 1):
            for to in range(CHAIN):
                if to == at:
                    continue
                lag = PASSED[at, to]

                @pl.when((link == at) & (step >= lag) & (step < chunks + lag))
                def _():
                    where = jnp.int32(to)
                    arrive(step - lag, where, to > at)
                    send(step - lag, where, to > at)

    def close(chunk):
        @pl.when(link > 0)
        def _():
            arrive_own(chunk, True)

        @pl.when(link < CHAIN - 1)
        def _():
            arrive_own(chunk, False)

        coeffs, variance = finish([part[chunk, link, k] for k in range(SUMS)])
        rows = pl.ds(pl.multiple_of(chunk * ROWS, ROWS), ROWS)
        for k in range(HARM):
            coeff_out[k, rows, :] = coeffs[k]
        var_out[rows, :] = variance

    def each_early(act):
        for chunk in range(early):
            for away in range(members):
                other = lax.rem(member + away, members)
                pl.when(chunk < early_of(other))(functools.partial(act, chunk, away, other))

    def send_early(chunk, away, other):
        own = early_raw.at[chunk, pl.ds(member * held, held)]
        pltpu.make_async_remote_copy(
            src_ref=stage.at[chunk, :, :, pl.ds(pl.multiple_of(other * LANES, LANES), LANES)],
            dst_ref=passing.at[chunk, away - 1] if away else own,
            send_sem=raw_send if away else early_send,
            recv_sem=(passing_recv if away else early_recv).at[chunk],
            device_id=device(inner, member),
            device_id_type=MESH,
        ).start()

    def forward_early(chunk, away, other):
        if away:
            pltpu.make_async_remote_copy(
                src_ref=passing.at[chunk, away - 1],
                dst_ref=early_raw.at[chunk, pl.ds(member * held, held)],
                send_sem=early_send,
                recv_sem=early_recv.at[chunk],
                device_id=device(link, other),
                device_id_type=MESH,
            ).start()

    def wait_passed(sem_of):
        for chunk in range(early):
            even, odd = chunk < EARLY_EVEN, chunk < EARLY_ODD
            for parity in range(2):
                pieces = members // 2 * (even + odd) - (odd if parity else even)

                @pl.when(lax.rem(member, 2) == parity)
                def _():
                    got = passing.at[chunk, pl.ds(0, pieces)]
                    pltpu.make_async_copy(got, got, sem_of(chunk)).wait()

    def forward():
        wait_passed(lambda chunk: passing_recv.at[chunk])
        each_early(forward_early)

    if direct:
        pltpu.make_async_copy(first_stage, first_stage, stage_sem.at[0]).wait()
        for parity in (1, 0):
            for away in range(1, members):
                spread_first = functools.partial(
                    spread_one, jnp.int32(0), first_to, away, 0, held, member * held, first_stage
                )
                pl.when(lax.rem(member + away, 2) == parity)(spread_first)
        spread_one(jnp.int32(0), first_to, 0, 0)

        @pl.when(at_end)
        def _():
            for chunk in range(early):
                pltpu.make_async_copy(stage.at[chunk], stage.at[chunk], stage_sem.at[1 + chunk]).wait()
            each_early(send_early)

    lax.fori_loop(0, AHEAD, lambda step, _: (spread(step), 0)[1], 0)
    if early:

        @pl.when(at_end)
        def _():
            for chunk in range(EARLY):
                for away in range(members):
                    other = lax.rem(member + away, members)
                    pl.when(chunk >= early_of(other))(functools.partial(spread_one, chunk, inner, away, chunk * ROWS))
    close_lag = by_link(CLOSE)

    def body(step, carry):
        spread(step + AHEAD)
        each(step, add_up, skip=own_early if early else 0)
        relay(step)
        if early:
            pl.when((step == FORWARD) & ~at_end)(forward)

        @pl.when((step >= close_lag) & (step < chunks + close_lag))
        def _():
            close(step - close_lag)

        return carry

    lax.fori_loop(0, chunks + max(PASSED.values()), body, 0)

    lons = pl.ds(0, (members - 1) * CHAIN * LANES)
    sent = field.at[:, :, lons] if local_rows % lat == 0 else field.at[:, lons]
    pltpu.make_async_copy(sent, sent, raw_send).wait()
    passed = part.at[pl.ds(early, chunks - early), pl.ds(0, CHAIN - 1)]
    pltpu.make_async_copy(passed, passed, part_send).wait()
    if early:
        passed = part.at[pl.ds(0, early), pl.ds(0, CHAIN - 2)]
        pltpu.make_async_copy(passed, passed, part_send).wait()

        @pl.when(at_end)
        def _():
            for chunk in range(early):

                @pl.when(chunk < own_early)
                def _():
                    own = early_raw.at[chunk, pl.ds(0, held)]
                    pltpu.make_async_copy(own, own, early_send).wait()

                @pl.when(chunk >= own_early)
                def _():
                    passed = part.at[chunk, 0]
                    pltpu.make_async_copy(passed, passed, part_send).wait()

        @pl.when(~at_end)
        def _():
            passed = part.at[pl.ds(0, early), 0]
            pltpu.make_async_copy(passed, passed, part_send).wait()
            wait_passed(lambda chunk: early_send)


def scoped(groups, lat, local_rows, field, coeff_out, var_out, raw, part, below, above, *direct):
    chunks = lat // ROWS
    sems = [
        pltpu.SemaphoreType.DMA,
        pltpu.SemaphoreType.DMA((chunks, CHAIN)),
        pltpu.SemaphoreType.DMA,
        pltpu.SemaphoreType.DMA((chunks, CHAIN + 1)),
    ]
    if direct:
        sems += [
            pltpu.SemaphoreType.DMA((1 + EARLY,)),
            pltpu.SemaphoreType.DMA((EARLY,)),
            pltpu.SemaphoreType.DMA((EARLY,)),
            pltpu.SemaphoreType.DMA,
        ]
    pl.run_scoped(
        functools.partial(
            kernel, groups, lat, local_rows, field, coeff_out, var_out, raw, part, below, above, direct
        ),
        *sems,
    )


def put_out(coeffs, variance, coeff_out, var_out, sem):
    copies = [
        pltpu.make_async_copy(coeffs, coeff_out, sem.at[0]),
        pltpu.make_async_copy(variance, var_out, sem.at[1]),
    ]
    for copy in copies:
        copy.start()
    for copy in copies:
        copy.wait()


def local(snapshots):
    groups = lax.axis_size("io")
    local_rows, width = snapshots.shape
    lat = local_rows * groups // TIMES
    if width != groups * LANES or lat % ROWS or local_rows % ROWS or groups % CHAIN:
        raise ValueError("unsupported sizes")
    chunks = lat // ROWS
    members = groups // CHAIN
    held, whole = local_rows // lat, local_rows % lat == 0
    field = snapshots.reshape(held, lat, width) if whole else snapshots
    direct = [
        pltpu.VMEM((EARLY, held, ROWS, members * LANES), jnp.float32),
        pltpu.VMEM((held, ROWS, members * LANES), jnp.float32),
        pltpu.VMEM((EARLY, members - 1, held, ROWS, LANES), jnp.float32),
        pltpu.VMEM((EARLY, SPAN, ROWS, LANES), jnp.float32),
    ]
    results = pl.pallas_call(
        functools.partial(scoped, groups, lat, local_rows),
        out_shape=(
            jax.ShapeDtypeStruct((HARM, lat, LANES), jnp.float32),
            jax.ShapeDtypeStruct((lat, LANES), jnp.float32),
        ),
        in_specs=[pl.BlockSpec(memory_space=pl.ANY)],
        out_specs=(pl.BlockSpec(memory_space=pltpu.VMEM), pl.BlockSpec(memory_space=pltpu.VMEM)),
        scratch_shapes=[
            pltpu.VMEM((chunks, CHAIN, SPAN, ROWS, LANES), jnp.float32),
            pltpu.VMEM((chunks, CHAIN, SUMS, ROWS, LANES), jnp.float32),
            pltpu.VMEM((chunks, CHAIN, SUMS, ROWS, LANES), jnp.float32),
            pltpu.VMEM((chunks, CHAIN, SUMS, ROWS, LANES), jnp.float32),
            *(direct if whole else []),
        ],
        compiler_params=pltpu.CompilerParams(
            collective_id=0, has_side_effects=True, vmem_limit_bytes=44 * 2**20
        ),
        name="climatology",
    )(field)
    return pl.pallas_call(
        put_out,
        out_shape=tuple(jax.ShapeDtypeStruct(r.shape, r.dtype) for r in results),
        in_specs=[pl.BlockSpec(memory_space=pltpu.VMEM)] * 2,
        out_specs=(pl.BlockSpec(memory_space=pl.ANY),) * 2,
        scratch_shapes=[pltpu.SemaphoreType.DMA((2,))],
        compiler_params=pltpu.CompilerParams(vmem_limit_bytes=4 * 2**20),
        name="put_out",
    )(*results)


def solution(mesh):
    return jax.shard_map(
        local,
        mesh=mesh,
        in_specs=(P(("rep", "io"), None),),
        out_specs=(P("rep", None, "io"), P("rep", "io")),
        check_vma=False,
    )
```

```python
import functools

import jax
import jax.numpy as jnp
import numpy as np
from jax import lax
from jax.experimental import pallas as pl
from jax.experimental.pallas import tpu as pltpu
from jax.sharding import PartitionSpec as P

TIMES = 96
HARM = 16
MONTHS = 12
SPAN = 24
CHAIN = TIMES // SPAN
SLOW = 4
SUMS = MONTHS + SLOW + 1
LANES = 128
ROWS = 8
AHEAD = 4
SKEW = 3
EARLY_EVEN, EARLY_ODD = 2, 1
EARLY = max(EARLY_EVEN, EARLY_ODD)
FORWARD = 2
MESH = pl.DeviceIdType.MESH


def schedule():
    orders, added = [], []
    for at in range(CHAIN):
        far = sorted((to for to in range(CHAIN) if to != at), key=lambda to: -abs(to - at))
        lags = {at: SKEW * (CHAIN - 2)}
        for to in far:
            side = [other for other in far if (other > at) == (to > at)]
            lags[to] = SKEW * side.index(to)
        orders.append(far + [at])
        added.append(lags)
    passed, close = {}, []
    for to in range(CHAIN):
        for way in (range(to + 1), range(CHAIN - 1, to - 1, -1)):
            lag = -1
            for at in way:
                lag = max(added[at][to], lag + 1)
                passed[at, to] = max(lag, passed.get((at, to), 0))
        close.append(passed[to, to])
    return orders, added, passed, close


ORDERS, ADDED, PASSED, CLOSE = schedule()


def fit_constants():
    steps = np.arange(TIMES, dtype=np.float64)
    slow = np.stack(
        [
            (steps - (TIMES - 1) / 2.0) / (TIMES / 2.0),
            np.cos(2.0 * np.pi * steps / TIMES),
            np.sin(2.0 * np.pi * steps / TIMES),
            np.cos(4.0 * np.pi * steps / TIMES),
        ],
        axis=1,
    )
    month = np.arange(MONTHS, dtype=np.float64)
    angles = 2.0 * np.pi * month / MONTHS
    periodic = [np.cos(j * angles) for j in range(7)] + [np.sin(j * angles) for j in range(1, 6)]
    unmix = np.linalg.inv(np.stack(periodic, axis=1))
    years = TIMES // MONTHS
    cross = slow.reshape(years, MONTHS, SLOW).sum(axis=0)
    inner = np.linalg.inv(slow.T @ slow - cross.T @ cross / years)
    return slow, cross, inner, unmix, years


def dot(weights, values):
    total = None
    for weight, value in zip(weights, values):
        term = value * np.float32(weight)
        total = term if total is None else total + term
    return total


def finish(sums):
    _, cross, inner, unmix, years = fit_constants()
    by_month, moments, squares = sums[:MONTHS], sums[MONTHS : MONTHS + SLOW], sums[-1]
    reduced = [moments[k] - dot(cross[:, k] / years, by_month) for k in range(SLOW)]
    slow = [dot(inner[k], reduced) for k in range(SLOW)]
    level = [(by_month[m] - dot(cross[m], slow)) * np.float32(1.0 / years) for m in range(MONTHS)]
    explained = slow[0] * moments[0]
    for k in range(1, SLOW):
        explained = explained + slow[k] * moments[k]
    for m in range(MONTHS):
        explained = explained + level[m] * by_month[m]
    half = MONTHS // 2
    even = [level[0]] + [level[m] + level[MONTHS - m] for m in range(1, half)] + [level[half]]
    odd = [level[m] - level[MONTHS - m] for m in range(1, half)]
    cosines = [dot(unmix[j, : half + 1], even) for j in range(half + 1)]
    sines = [dot(unmix[half + j, 1:half], odd) for j in range(1, half)]
    coeffs = [cosines[0], slow[0]] + cosines[1:] + sines + slow[1:]
    return coeffs, (squares - explained) * np.float32(1.0 / TIMES)


def kernel(
    groups, lat, local_rows,
    field, coeff_out, var_out,
    raw, part, below, above, direct,
    raw_send, raw_recv, part_send, box_recv, *direct_sems,
):
    members = groups // CHAIN
    chunks = lat // ROWS
    held = local_rows // lat
    early = EARLY if direct else 0
    if direct:
        stage, first_stage, passing, early_raw = direct
        stage_sem, passing_recv, early_recv, early_send = direct_sems
    me = lax.axis_index("io")
    link, member = me // members, lax.rem(me, members)
    device = lambda at, who: {"io": at * members + who}

    span = fit_constants()[0][:SPAN]
    at_end = (link == 0) | (link == CHAIN - 1)
    early_of = lambda who: EARLY_ODD + (EARLY_EVEN - EARLY_ODD) * (1 - lax.rem(who, 2))
    own_early = early_of(member)
    def by_link(values):
        return sum((link == at).astype(jnp.int32) * values[at] for at in range(CHAIN))

    inner = by_link([1, 0, CHAIN - 1, CHAIN - 2])

    def block_of(chunk, to):
        lons = pl.ds(pl.multiple_of(to * members * LANES, LANES), members * LANES)
        return field.at[:, pl.ds(chunk * ROWS, ROWS), lons]

    barrier = pltpu.get_barrier_semaphore()
    for step in range(1, members):
        other = lax.rem(member + step, members)
        pl.semaphore_signal(barrier, inc=1, device_id=device(link, other), device_id_type=MESH)

    @pl.when(link > 0)
    def _():
        pl.semaphore_signal(barrier, inc=1, device_id=device(link - 1, member), device_id_type=MESH)

    @pl.when(link < CHAIN - 1)
    def _():
        pl.semaphore_signal(barrier, inc=1, device_id=device(link + 1, member), device_id_type=MESH)

    first_to = by_link([ORDERS[at][0] for at in range(CHAIN)])
    if direct:
        pltpu.make_async_copy(block_of(0, first_to), first_stage, stage_sem.at[0]).start()

        @pl.when(at_end)
        def _():
            for chunk in range(early):
                pltpu.make_async_copy(block_of(chunk, inner), stage.at[chunk], stage_sem.at[1 + chunk]).start()

    ends = (link == 0).astype(jnp.int32) + (link == CHAIN - 1).astype(jnp.int32)
    pl.semaphore_wait(barrier, members + 1 - ends)

    def spread_one(chunk, to, step, row, count=held, time=None, staged=None):
        other = lax.rem(member + step, members)
        time = member * held if time is None else time
        lon = pl.multiple_of((to * members + other) * LANES, LANES)
        if count is None:
            src = field.at[pl.ds(row, ROWS), pl.ds(lon, LANES)]
            dst = raw.at[chunk, to, time]
        else:
            src = field.at[:, pl.ds(row, ROWS), pl.ds(lon, LANES)]
            if staged is not None and step > 0:
                src = staged.at[:, :, pl.ds(pl.multiple_of(other * LANES, LANES), LANES)]
            dst = raw.at[chunk, to, pl.ds(time, count)]
        arrived = raw_recv.at[chunk, to]
        if step == 0:
            pltpu.make_async_copy(src, dst, arrived).start()
        else:
            pltpu.make_async_remote_copy(
                src_ref=src, dst_ref=dst, send_sem=raw_send, recv_sem=arrived,
                device_id=device(link, other), device_id_type=MESH,
            ).start()

    def spread_rows(*where):
        for step in list(range(1, members)) + [0]:
            spread_one(where[0], where[1], step, *where[2:])

    def spread_block(chunk, to):
        if local_rows % lat == 0:
            count = local_rows // lat
            spread_rows(chunk, to, pl.multiple_of(chunk * ROWS, ROWS), count, member * count)
        else:
            first = member * local_rows
            for extra in range(local_rows // lat + 2):
                time = first // lat + extra
                row = time * lat + chunk * ROWS - first

                @pl.when((row >= 0) & (row < local_rows))
                def _():
                    spread_rows(chunk, to, pl.multiple_of(row, ROWS), None, time)

    def each(step, act, staged_first=False, skip=0):
        for rank in range(CHAIN):
            lag = by_link([ADDED[at][ORDERS[at][rank]] for at in range(CHAIN)])

            to = by_link([ORDERS[at][rank] for at in range(CHAIN)])
            begin = lag + 1 if staged_first and rank == 0 else lag

            @pl.when((step >= begin) & (step < chunks + lag) & ((step >= lag + skip) | ~at_end | (to != inner)))
            def _():
                act(step - lag, to)

    def spread(step):
        each(step, spread_block, staged_first=bool(direct), skip=early)

    def box_sem(chunk, to, up, at):
        where = to if up else to + (to == at).astype(jnp.int32) * (CHAIN - to)
        return box_recv.at[chunk, where]

    def send(chunk, to, up):
        at = link + 1 if up else link - 1
        pltpu.make_async_remote_copy(
            src_ref=part.at[chunk, to],
            dst_ref=(below if up else above).at[chunk, to],
            send_sem=part_send,
            recv_sem=box_sem(chunk, to, up, at),
            device_id=device(at, member),
            device_id_type=MESH,
        ).start()

    def take(chunk, to, box):
        for k in range(SUMS):
            part[chunk, to, k] = part[chunk, to, k] + box[chunk, to, k]

    def wait_box(chunk, to, up):
        box = below if up else above
        pltpu.make_async_copy(box.at[chunk, to], box.at[chunk, to], box_sem(chunk, to, up, link)).wait()

    def arrive(chunk, to, up):
        wait_box(chunk, to, up)
        take(chunk, to, below if up else above)

    def arrive_own(chunk, up):
        if early:
            stands_in = (link == (1 if up else CHAIN - 2)) & (chunk < own_early)

            @pl.when(stands_in)
            def _():
                got = early_raw.at[chunk]
                pltpu.make_async_copy(got, got, early_recv.at[chunk]).wait()
                sum_span(lambda time: early_raw[chunk, time], inner, below if up else above, chunk, link)

            @pl.when(~stands_in)
            def _():
                wait_box(chunk, link, up)

        else:
            wait_box(chunk, link, up)
        take(chunk, link, below if up else above)

    def sum_span(value_at, source, result, chunk, to):
        offset = source.astype(jnp.float32) * np.float32(SPAN / (TIMES / 2.0))
        quarter = lambda at: (source == at).astype(jnp.float32)
        turn_cos, turn_sin = quarter(0) - quarter(2), quarter(1) - quarter(3)
        flip = quarter(0) - quarter(1) + quarter(2) - quarter(3)
        local = [None] * (SLOW + 1)
        whole = None
        for month in range(MONTHS):
            kept = None
            for time in range(month, SPAN, MONTHS):
                value = value_at(time)
                kept = value if kept is None else kept + value
                terms = [value * np.float32(span[time, k]) for k in range(SLOW)] + [value * value]
                local = [term if own is None else own + term for own, term in zip(local, terms)]
            result[chunk, to, month] = kept
            whole = kept if whole is None else whole + kept
        trend, cosine, sine, double, squares = local
        result[chunk, to, MONTHS] = trend + whole * offset
        result[chunk, to, MONTHS + 1] = cosine * turn_cos - sine * turn_sin
        result[chunk, to, MONTHS + 2] = cosine * turn_sin + sine * turn_cos
        result[chunk, to, MONTHS + 3] = double * flip
        result[chunk, to, MONTHS + 4] = squares

    def add_up(chunk, to):
        pltpu.make_async_copy(
            raw.at[chunk, to], raw.at[chunk, to], raw_recv.at[chunk, to]
        ).wait()
        sum_span(lambda time: raw[chunk, to, time], link, part, chunk, to)

        @pl.when((link == 0) & (to > 0))
        def _():
            send(chunk, to, True)

        @pl.when((link == CHAIN - 1) & (to < CHAIN - 1))
        def _():
            send(chunk, to, False)

    def relay(step):
        for at in range(1, CHAIN - 1):
            for to in range(CHAIN):
                if to == at:
                    continue
                lag = PASSED[at, to]

                @pl.when((link == at) & (step >= lag) & (step < chunks + lag))
                def _():
                    where = jnp.int32(to)
                    arrive(step - lag, where, to > at)
                    send(step - lag, where, to > at)

    def close(chunk):
        @pl.when(link > 0)
        def _():
            arrive_own(chunk, True)

        @pl.when(link < CHAIN - 1)
        def _():
            arrive_own(chunk, False)

        coeffs, variance = finish([part[chunk, link, k] for k in range(SUMS)])
        rows = pl.ds(pl.multiple_of(chunk * ROWS, ROWS), ROWS)
        for k in range(HARM):
            coeff_out[k, rows, :] = coeffs[k]
        var_out[rows, :] = variance

    def each_early(act):
        for chunk in range(early):
            for away in range(members):
                other = lax.rem(member + away, members)
                pl.when(chunk < early_of(other))(functools.partial(act, chunk, away, other))

    def send_early(chunk, away, other):
        own = early_raw.at[chunk, pl.ds(member * held, held)]
        pltpu.make_async_remote_copy(
            src_ref=stage.at[chunk, :, :, pl.ds(pl.multiple_of(other * LANES, LANES), LANES)],
            dst_ref=passing.at[chunk, away - 1] if away else own,
            send_sem=raw_send if away else early_send,
            recv_sem=(passing_recv if away else early_recv).at[chunk],
            device_id=device(inner, member),
            device_id_type=MESH,
        ).start()

    def forward_early(chunk, away, other):
        if away:
            pltpu.make_async_remote_copy(
                src_ref=passing.at[chunk, away - 1],
                dst_ref=early_raw.at[chunk, pl.ds(member * held, held)],
                send_sem=early_send,
                recv_sem=early_recv.at[chunk],
                device_id=device(link, other),
                device_id_type=MESH,
            ).start()

    def wait_passed(sem_of):
        for chunk in range(early):
            even, odd = chunk < EARLY_EVEN, chunk < EARLY_ODD
            for parity in range(2):
                pieces = members // 2 * (even + odd) - (odd if parity else even)

                @pl.when(lax.rem(member, 2) == parity)
                def _():
                    got = passing.at[chunk, pl.ds(0, pieces)]
                    pltpu.make_async_copy(got, got, sem_of(chunk)).wait()

    def forward():
        wait_passed(lambda chunk: passing_recv.at[chunk])
        each_early(forward_early)

    if direct:
        pltpu.make_async_copy(first_stage, first_stage, stage_sem.at[0]).wait()
        for parity in (1, 0):
            for away in range(1, members):
                spread_first = functools.partial(
                    spread_one, jnp.int32(0), first_to, away, 0, held, member * held, first_stage
                )
                pl.when(lax.rem(member + away, 2) == parity)(spread_first)
        spread_one(jnp.int32(0), first_to, 0, 0)

        @pl.when(at_end)
        def _():
            for chunk in range(early):
                pltpu.make_async_copy(stage.at[chunk], stage.at[chunk], stage_sem.at[1 + chunk]).wait()
            each_early(send_early)

    lax.fori_loop(0, AHEAD, lambda step, _: (spread(step), 0)[1], 0)
    close_lag = by_link(CLOSE)

    def body(step, carry):
        spread(step + AHEAD)
        if early:

            @pl.when(at_end & (step == SKEW))
            def _():
                for chunk in range(EARLY):
                    for away in range(members):
                        other = lax.rem(member + away, members)
                        pl.when(chunk >= early_of(other))(functools.partial(spread_one, chunk, inner, away, chunk * ROWS))

        each(step, add_up, skip=own_early if early else 0)
        relay(step)
        if early:
            pl.when((step == FORWARD) & ~at_end)(forward)

        @pl.when((step >= close_lag) & (step < chunks + close_lag))
        def _():
            close(step - close_lag)

        return carry

    lax.fori_loop(0, chunks + max(PASSED.values()), body, 0)

    lons = pl.ds(0, (members - 1) * CHAIN * LANES)
    sent = field.at[:, :, lons] if local_rows % lat == 0 else field.at[:, lons]
    pltpu.make_async_copy(sent, sent, raw_send).wait()
    passed = part.at[pl.ds(early, chunks - early), pl.ds(0, CHAIN - 1)]
    pltpu.make_async_copy(passed, passed, part_send).wait()
    if early:
        passed = part.at[pl.ds(0, early), pl.ds(0, CHAIN - 2)]
        pltpu.make_async_copy(passed, passed, part_send).wait()

        @pl.when(at_end)
        def _():
            for chunk in range(early):

                @pl.when(chunk < own_early)
                def _():
                    own = early_raw.at[chunk, pl.ds(0, held)]
                    pltpu.make_async_copy(own, own, early_send).wait()

                @pl.when(chunk >= own_early)
                def _():
                    passed = part.at[chunk, 0]
                    pltpu.make_async_copy(passed, passed, part_send).wait()

        @pl.when(~at_end)
        def _():
            passed = part.at[pl.ds(0, early), 0]
            pltpu.make_async_copy(passed, passed, part_send).wait()
            wait_passed(lambda chunk: early_send)


def scoped(groups, lat, local_rows, field, coeff_out, var_out, raw, part, below, above, *direct):
    chunks = lat // ROWS
    sems = [
        pltpu.SemaphoreType.DMA,
        pltpu.SemaphoreType.DMA((chunks, CHAIN)),
        pltpu.SemaphoreType.DMA,
        pltpu.SemaphoreType.DMA((chunks, CHAIN + 1)),
    ]
    if direct:
        sems += [
            pltpu.SemaphoreType.DMA((1 + EARLY,)),
            pltpu.SemaphoreType.DMA((EARLY,)),
            pltpu.SemaphoreType.DMA((EARLY,)),
            pltpu.SemaphoreType.DMA,
        ]
    pl.run_scoped(
        functools.partial(
            kernel, groups, lat, local_rows, field, coeff_out, var_out, raw, part, below, above, direct
        ),
        *sems,
    )


def put_out(coeffs, variance, coeff_out, var_out, sem):
    copies = [
        pltpu.make_async_copy(coeffs, coeff_out, sem.at[0]),
        pltpu.make_async_copy(variance, var_out, sem.at[1]),
    ]
    for copy in copies:
        copy.start()
    for copy in copies:
        copy.wait()


def local(snapshots):
    groups = lax.axis_size("io")
    local_rows, width = snapshots.shape
    lat = local_rows * groups // TIMES
    if width != groups * LANES or lat % ROWS or local_rows % ROWS or groups % CHAIN:
        raise ValueError("unsupported sizes")
    chunks = lat // ROWS
    members = groups // CHAIN
    held, whole = local_rows // lat, local_rows % lat == 0
    field = snapshots.reshape(held, lat, width) if whole else snapshots
    direct = [
        pltpu.VMEM((EARLY, held, ROWS, members * LANES), jnp.float32),
        pltpu.VMEM((held, ROWS, members * LANES), jnp.float32),
        pltpu.VMEM((EARLY, members - 1, held, ROWS, LANES), jnp.float32),
        pltpu.VMEM((EARLY, SPAN, ROWS, LANES), jnp.float32),
    ]
    results = pl.pallas_call(
        functools.partial(scoped, groups, lat, local_rows),
        out_shape=(
            jax.ShapeDtypeStruct((HARM, lat, LANES), jnp.float32),
            jax.ShapeDtypeStruct((lat, LANES), jnp.float32),
        ),
        in_specs=[pl.BlockSpec(memory_space=pl.ANY)],
        out_specs=(pl.BlockSpec(memory_space=pltpu.VMEM), pl.BlockSpec(memory_space=pltpu.VMEM)),
        scratch_shapes=[
            pltpu.VMEM((chunks, CHAIN, SPAN, ROWS, LANES), jnp.float32),
            pltpu.VMEM((chunks, CHAIN, SUMS, ROWS, LANES), jnp.float32),
            pltpu.VMEM((chunks, CHAIN, SUMS, ROWS, LANES), jnp.float32),
            pltpu.VMEM((chunks, CHAIN, SUMS, ROWS, LANES), jnp.float32),
            *(direct if whole else []),
        ],
        compiler_params=pltpu.CompilerParams(
            collective_id=0, has_side_effects=True, vmem_limit_bytes=44 * 2**20
        ),
        name="climatology",
    )(field)
    return pl.pallas_call(
        put_out,
        out_shape=tuple(jax.ShapeDtypeStruct(r.shape, r.dtype) for r in results),
        in_specs=[pl.BlockSpec(memory_space=pltpu.VMEM)] * 2,
        out_specs=(pl.BlockSpec(memory_space=pl.ANY),) * 2,
        scratch_shapes=[pltpu.SemaphoreType.DMA((2,))],
        compiler_params=pltpu.CompilerParams(vmem_limit_bytes=4 * 2**20),
        name="put_out",
    )(*results)


def solution(mesh):
    return jax.shard_map(
        local,
        mesh=mesh,
        in_specs=(P(("rep", "io"), None),),
        out_specs=(P("rep", None, "io"), P("rep", "io")),
        check_vma=False,
    )
```

```python
import functools

import jax
import jax.numpy as jnp
import numpy as np
from jax import lax
from jax.experimental import pallas as pl
from jax.experimental.pallas import tpu as pltpu
from jax.sharding import PartitionSpec as P

TIMES = 96
HARM = 16
MONTHS = 12
SPAN = 24
CHAIN = TIMES // SPAN
SLOW = 4
SUMS = MONTHS + SLOW + 1
LANES = 128
ROWS = 8
AHEAD = 4
SKEW = 3
EARLY_EVEN, EARLY_ODD = 2, 1
EARLY = max(EARLY_EVEN, EARLY_ODD)
FORWARD = 2
MESH = pl.DeviceIdType.MESH


def schedule():
    orders, added = [], []
    for at in range(CHAIN):
        far = sorted((to for to in range(CHAIN) if to != at), key=lambda to: -abs(to - at))
        lags = {at: SKEW * (CHAIN - 2)}
        for to in far:
            side = [other for other in far if (other > at) == (to > at)]
            lags[to] = SKEW * side.index(to)
        orders.append(sorted(far, key=lags.get) + [at])
        added.append(lags)
    passed, close = {}, []
    for to in range(CHAIN):
        for way in (range(to + 1), range(CHAIN - 1, to - 1, -1)):
            lag = -1
            for at in way:
                lag = max(added[at][to], lag + 1)
                passed[at, to] = max(lag, passed.get((at, to), 0))
        close.append(passed[to, to])
    return orders, added, passed, close


ORDERS, ADDED, PASSED, CLOSE = schedule()


def fit_constants():
    steps = np.arange(TIMES, dtype=np.float64)
    slow = np.stack(
        [
            (steps - (TIMES - 1) / 2.0) / (TIMES / 2.0),
            np.cos(2.0 * np.pi * steps / TIMES),
            np.sin(2.0 * np.pi * steps / TIMES),
            np.cos(4.0 * np.pi * steps / TIMES),
        ],
        axis=1,
    )
    month = np.arange(MONTHS, dtype=np.float64)
    angles = 2.0 * np.pi * month / MONTHS
    periodic = [np.cos(j * angles) for j in range(7)] + [np.sin(j * angles) for j in range(1, 6)]
    unmix = np.linalg.inv(np.stack(periodic, axis=1))
    years = TIMES // MONTHS
    cross = slow.reshape(years, MONTHS, SLOW).sum(axis=0)
    inner = np.linalg.inv(slow.T @ slow - cross.T @ cross / years)
    return slow, cross, inner, unmix, years


def dot(weights, values):
    total = None
    for weight, value in zip(weights, values):
        term = value * np.float32(weight)
        total = term if total is None else total + term
    return total


def finish(sums):
    _, cross, inner, unmix, years = fit_constants()
    by_month, moments, squares = sums[:MONTHS], sums[MONTHS : MONTHS + SLOW], sums[-1]
    reduced = [moments[k] - dot(cross[:, k] / years, by_month) for k in range(SLOW)]
    slow = [dot(inner[k], reduced) for k in range(SLOW)]
    level = [(by_month[m] - dot(cross[m], slow)) * np.float32(1.0 / years) for m in range(MONTHS)]
    explained = slow[0] * moments[0]
    for k in range(1, SLOW):
        explained = explained + slow[k] * moments[k]
    for m in range(MONTHS):
        explained = explained + level[m] * by_month[m]
    half = MONTHS // 2
    even = [level[0]] + [level[m] + level[MONTHS - m] for m in range(1, half)] + [level[half]]
    odd = [level[m] - level[MONTHS - m] for m in range(1, half)]
    cosines = [dot(unmix[j, : half + 1], even) for j in range(half + 1)]
    sines = [dot(unmix[half + j, 1:half], odd) for j in range(1, half)]
    coeffs = [cosines[0], slow[0]] + cosines[1:] + sines + slow[1:]
    return coeffs, (squares - explained) * np.float32(1.0 / TIMES)


def kernel(
    groups, lat, local_rows,
    field, coeff_out, var_out,
    raw, part, below, above, direct,
    raw_send, raw_recv, part_send, box_recv, *direct_sems,
):
    members = groups // CHAIN
    chunks = lat // ROWS
    held = local_rows // lat
    early = EARLY if direct else 0
    if direct:
        stage, first_stage, passing, early_raw = direct
        stage_sem, passing_recv, early_recv, early_send = direct_sems
    me = lax.axis_index("io")
    link, member = me // members, lax.rem(me, members)
    device = lambda at, who: {"io": at * members + who}

    span = fit_constants()[0][:SPAN]
    at_end = (link == 0) | (link == CHAIN - 1)
    early_of = lambda who: EARLY_ODD + (EARLY_EVEN - EARLY_ODD) * (1 - lax.rem(who, 2))
    own_early = early_of(member)
    def by_link(values):
        return sum((link == at).astype(jnp.int32) * values[at] for at in range(CHAIN))

    inner = by_link([1, 0, CHAIN - 1, CHAIN - 2])

    def block_of(chunk, to):
        lons = pl.ds(pl.multiple_of(to * members * LANES, LANES), members * LANES)
        return field.at[:, pl.ds(chunk * ROWS, ROWS), lons]

    barrier = pltpu.get_barrier_semaphore()
    for step in range(1, members):
        other = lax.rem(member + step, members)
        pl.semaphore_signal(barrier, inc=1, device_id=device(link, other), device_id_type=MESH)

    @pl.when(link > 0)
    def _():
        pl.semaphore_signal(barrier, inc=1, device_id=device(link - 1, member), device_id_type=MESH)

    @pl.when(link < CHAIN - 1)
    def _():
        pl.semaphore_signal(barrier, inc=1, device_id=device(link + 1, member), device_id_type=MESH)

    first_to = by_link([ORDERS[at][0] for at in range(CHAIN)])
    if direct:
        pltpu.make_async_copy(block_of(0, first_to), first_stage, stage_sem.at[0]).start()

        @pl.when(at_end)
        def _():
            for chunk in range(early):
                pltpu.make_async_copy(block_of(chunk, inner), stage.at[chunk], stage_sem.at[1 + chunk]).start()

    ends = (link == 0).astype(jnp.int32) + (link == CHAIN - 1).astype(jnp.int32)
    pl.semaphore_wait(barrier, members + 1 - ends)

    def spread_one(chunk, to, step, row, count=held, time=None, staged=None):
        other = lax.rem(member + step, members)
        time = member * held if time is None else time
        lon = pl.multiple_of((to * members + other) * LANES, LANES)
        if count is None:
            src = field.at[pl.ds(row, ROWS), pl.ds(lon, LANES)]
            dst = raw.at[chunk, to, time]
        else:
            src = field.at[:, pl.ds(row, ROWS), pl.ds(lon, LANES)]
            if staged is not None and step > 0:
                src = staged.at[:, :, pl.ds(pl.multiple_of(other * LANES, LANES), LANES)]
            dst = raw.at[chunk, to, pl.ds(time, count)]
        arrived = raw_recv.at[chunk, to]
        if step == 0:
            pltpu.make_async_copy(src, dst, arrived).start()
        else:
            pltpu.make_async_remote_copy(
                src_ref=src, dst_ref=dst, send_sem=raw_send, recv_sem=arrived,
                device_id=device(link, other), device_id_type=MESH,
            ).start()

    def spread_rows(*where):
        for step in list(range(1, members)) + [0]:
            spread_one(where[0], where[1], step, *where[2:])

    def spread_block(chunk, to):
        if local_rows % lat == 0:
            count = local_rows // lat
            spread_rows(chunk, to, pl.multiple_of(chunk * ROWS, ROWS), count, member * count)
        else:
            first = member * local_rows
            for extra in range(local_rows // lat + 2):
                time = first // lat + extra
                row = time * lat + chunk * ROWS - first

                @pl.when((row >= 0) & (row < local_rows))
                def _():
                    spread_rows(chunk, to, pl.multiple_of(row, ROWS), None, time)

    def each(step, act, staged_first=False, skip=0):
        for rank in range(CHAIN):
            lag = by_link([ADDED[at][ORDERS[at][rank]] for at in range(CHAIN)])

            to = by_link([ORDERS[at][rank] for at in range(CHAIN)])
            begin = lag + 1 if staged_first and rank == 0 else lag

            @pl.when((step >= begin) & (step < chunks + lag) & ((step >= lag + skip) | ~at_end | (to != inner)))
            def _():
                act(step - lag, to)

    def spread(step):
        each(step, spread_block, staged_first=bool(direct), skip=early)

    def box_sem(chunk, to, up, at):
        where = to if up else to + (to == at).astype(jnp.int32) * (CHAIN - to)
        return box_recv.at[chunk, where]

    def send(chunk, to, up):
        at = link + 1 if up else link - 1
        pltpu.make_async_remote_copy(
            src_ref=part.at[chunk, to],
            dst_ref=(below if up else above).at[chunk, to],
            send_sem=part_send,
            recv_sem=box_sem(chunk, to, up, at),
            device_id=device(at, member),
            device_id_type=MESH,
        ).start()

    def take(chunk, to, box):
        for k in range(SUMS):
            part[chunk, to, k] = part[chunk, to, k] + box[chunk, to, k]

    def wait_box(chunk, to, up):
        box = below if up else above
        pltpu.make_async_copy(box.at[chunk, to], box.at[chunk, to], box_sem(chunk, to, up, link)).wait()

    def arrive(chunk, to, up):
        wait_box(chunk, to, up)
        take(chunk, to, below if up else above)

    def arrive_own(chunk, up):
        if early:
            stands_in = (link == (1 if up else CHAIN - 2)) & (chunk < own_early)

            @pl.when(stands_in)
            def _():
                got = early_raw.at[chunk]
                pltpu.make_async_copy(got, got, early_recv.at[chunk]).wait()
                sum_span(lambda time: early_raw[chunk, time], inner, below if up else above, chunk, link)

            @pl.when(~stands_in)
            def _():
                wait_box(chunk, link, up)

        else:
            wait_box(chunk, link, up)
        take(chunk, link, below if up else above)

    def sum_span(value_at, source, result, chunk, to):
        offset = source.astype(jnp.float32) * np.float32(SPAN / (TIMES / 2.0))
        quarter = lambda at: (source == at).astype(jnp.float32)
        turn_cos, turn_sin = quarter(0) - quarter(2), quarter(1) - quarter(3)
        flip = quarter(0) - quarter(1) + quarter(2) - quarter(3)
        local = [None] * (SLOW + 1)
        whole = None
        for month in range(MONTHS):
            kept = None
            for time in range(month, SPAN, MONTHS):
                value = value_at(time)
                kept = value if kept is None else kept + value
                terms = [value * np.float32(span[time, k]) for k in range(SLOW)] + [value * value]
                local = [term if own is None else own + term for own, term in zip(local, terms)]
            result[chunk, to, month] = kept
            whole = kept if whole is None else whole + kept
        trend, cosine, sine, double, squares = local
        result[chunk, to, MONTHS] = trend + whole * offset
        result[chunk, to, MONTHS + 1] = cosine * turn_cos - sine * turn_sin
        result[chunk, to, MONTHS + 2] = cosine * turn_sin + sine * turn_cos
        result[chunk, to, MONTHS + 3] = double * flip
        result[chunk, to, MONTHS + 4] = squares

    def add_up(chunk, to):
        pltpu.make_async_copy(
            raw.at[chunk, to], raw.at[chunk, to], raw_recv.at[chunk, to]
        ).wait()
        sum_span(lambda time: raw[chunk, to, time], link, part, chunk, to)

        @pl.when((link == 0) & (to > 0))
        def _():
            send(chunk, to, True)

        @pl.when((link == CHAIN - 1) & (to < CHAIN - 1))
        def _():
            send(chunk, to, False)

    def relay(step):
        for at in range(1, CHAIN - 1):
            for to in range(CHAIN):
                if to == at:
                    continue
                lag = PASSED[at, to]

                @pl.when((link == at) & (step >= lag) & (step < chunks + lag))
                def _():
                    where = jnp.int32(to)
                    arrive(step - lag, where, to > at)
                    send(step - lag, where, to > at)

    def close(chunk):
        @pl.when(link > 0)
        def _():
            arrive_own(chunk, True)

        @pl.when(link < CHAIN - 1)
        def _():
            arrive_own(chunk, False)

        coeffs, variance = finish([part[chunk, link, k] for k in range(SUMS)])
        rows = pl.ds(pl.multiple_of(chunk * ROWS, ROWS), ROWS)
        for k in range(HARM):
            coeff_out[k, rows, :] = coeffs[k]
        var_out[rows, :] = variance

    def each_early(act):
        for chunk in range(early):
            for away in range(members):
                other = lax.rem(member + away, members)
                pl.when(chunk < early_of(other))(functools.partial(act, chunk, away, other))

    def send_early(chunk, away, other):
        own = early_raw.at[chunk, pl.ds(member * held, held)]
        pltpu.make_async_remote_copy(
            src_ref=stage.at[chunk, :, :, pl.ds(pl.multiple_of(other * LANES, LANES), LANES)],
            dst_ref=passing.at[chunk, away - 1] if away else own,
            send_sem=raw_send if away else early_send,
            recv_sem=(passing_recv if away else early_recv).at[chunk],
            device_id=device(inner, member),
            device_id_type=MESH,
        ).start()

    def forward_early(chunk, away, other):
        if away:
            pltpu.make_async_remote_copy(
                src_ref=passing.at[chunk, away - 1],
                dst_ref=early_raw.at[chunk, pl.ds(member * held, held)],
                send_sem=early_send,
                recv_sem=early_recv.at[chunk],
                device_id=device(link, other),
                device_id_type=MESH,
            ).start()

    def wait_passed(sem_of):
        for chunk in range(early):
            even, odd = chunk < EARLY_EVEN, chunk < EARLY_ODD
            for parity in range(2):
                pieces = members // 2 * (even + odd) - (odd if parity else even)

                @pl.when(lax.rem(member, 2) == parity)
                def _():
                    got = passing.at[chunk, pl.ds(0, pieces)]
                    pltpu.make_async_copy(got, got, sem_of(chunk)).wait()

    def forward():
        wait_passed(lambda chunk: passing_recv.at[chunk])
        each_early(forward_early)

    if direct:
        pltpu.make_async_copy(first_stage, first_stage, stage_sem.at[0]).wait()
        for parity in (1, 0):
            for away in range(1, members):
                spread_first = functools.partial(
                    spread_one, jnp.int32(0), first_to, away, 0, held, member * held, first_stage
                )
                pl.when(lax.rem(member + away, 2) == parity)(spread_first)
        spread_one(jnp.int32(0), first_to, 0, 0)

        @pl.when(at_end)
        def _():
            for chunk in range(early):
                pltpu.make_async_copy(stage.at[chunk], stage.at[chunk], stage_sem.at[1 + chunk]).wait()
            each_early(send_early)

    lax.fori_loop(0, AHEAD, lambda step, _: (spread(step), 0)[1], 0)
    close_lag = by_link(CLOSE)

    def body(step, carry):
        spread(step + AHEAD)
        if early:

            @pl.when(at_end & (step == SKEW))
            def _():
                for chunk in range(EARLY):
                    for away in range(members):
                        other = lax.rem(member + away, members)
                        pl.when(chunk >= early_of(other))(functools.partial(spread_one, chunk, inner, away, chunk * ROWS))

        each(step, add_up, skip=own_early if early else 0)
        relay(step)
        if early:
            pl.when((step == FORWARD) & ~at_end)(forward)

        @pl.when((step >= close_lag) & (step < chunks + close_lag))
        def _():
            close(step - close_lag)

        return carry

    lax.fori_loop(0, chunks + max(PASSED.values()), body, 0)

    lons = pl.ds(0, (members - 1) * CHAIN * LANES)
    sent = field.at[:, :, lons] if local_rows % lat == 0 else field.at[:, lons]
    pltpu.make_async_copy(sent, sent, raw_send).wait()
    passed = part.at[pl.ds(early, chunks - early), pl.ds(0, CHAIN - 1)]
    pltpu.make_async_copy(passed, passed, part_send).wait()
    if early:
        passed = part.at[pl.ds(0, early), pl.ds(0, CHAIN - 2)]
        pltpu.make_async_copy(passed, passed, part_send).wait()

        @pl.when(at_end)
        def _():
            for chunk in range(early):

                @pl.when(chunk < own_early)
                def _():
                    own = early_raw.at[chunk, pl.ds(0, held)]
                    pltpu.make_async_copy(own, own, early_send).wait()

                @pl.when(chunk >= own_early)
                def _():
                    passed = part.at[chunk, 0]
                    pltpu.make_async_copy(passed, passed, part_send).wait()

        @pl.when(~at_end)
        def _():
            passed = part.at[pl.ds(0, early), 0]
            pltpu.make_async_copy(passed, passed, part_send).wait()
            wait_passed(lambda chunk: early_send)


def scoped(groups, lat, local_rows, field, coeff_out, var_out, raw, part, below, above, *direct):
    chunks = lat // ROWS
    sems = [
        pltpu.SemaphoreType.DMA,
        pltpu.SemaphoreType.DMA((chunks, CHAIN)),
        pltpu.SemaphoreType.DMA,
        pltpu.SemaphoreType.DMA((chunks, CHAIN + 1)),
    ]
    if direct:
        sems += [
            pltpu.SemaphoreType.DMA((1 + EARLY,)),
            pltpu.SemaphoreType.DMA((EARLY,)),
            pltpu.SemaphoreType.DMA((EARLY,)),
            pltpu.SemaphoreType.DMA,
        ]
    pl.run_scoped(
        functools.partial(
            kernel, groups, lat, local_rows, field, coeff_out, var_out, raw, part, below, above, direct
        ),
        *sems,
    )


def put_out(coeffs, variance, coeff_out, var_out, sem):
    copies = [
        pltpu.make_async_copy(coeffs, coeff_out, sem.at[0]),
        pltpu.make_async_copy(variance, var_out, sem.at[1]),
    ]
    for copy in copies:
        copy.start()
    for copy in copies:
        copy.wait()


def local(snapshots):
    groups = lax.axis_size("io")
    local_rows, width = snapshots.shape
    lat = local_rows * groups // TIMES
    if width != groups * LANES or lat % ROWS or local_rows % ROWS or groups % CHAIN:
        raise ValueError("unsupported sizes")
    chunks = lat // ROWS
    members = groups // CHAIN
    held, whole = local_rows // lat, local_rows % lat == 0
    field = snapshots.reshape(held, lat, width) if whole else snapshots
    direct = [
        pltpu.VMEM((EARLY, held, ROWS, members * LANES), jnp.float32),
        pltpu.VMEM((held, ROWS, members * LANES), jnp.float32),
        pltpu.VMEM((EARLY, members - 1, held, ROWS, LANES), jnp.float32),
        pltpu.VMEM((EARLY, SPAN, ROWS, LANES), jnp.float32),
    ]
    results = pl.pallas_call(
        functools.partial(scoped, groups, lat, local_rows),
        out_shape=(
            jax.ShapeDtypeStruct((HARM, lat, LANES), jnp.float32),
            jax.ShapeDtypeStruct((lat, LANES), jnp.float32),
        ),
        in_specs=[pl.BlockSpec(memory_space=pl.ANY)],
        out_specs=(pl.BlockSpec(memory_space=pltpu.VMEM), pl.BlockSpec(memory_space=pltpu.VMEM)),
        scratch_shapes=[
            pltpu.VMEM((chunks, CHAIN, SPAN, ROWS, LANES), jnp.float32),
            pltpu.VMEM((chunks, CHAIN, SUMS, ROWS, LANES), jnp.float32),
            pltpu.VMEM((chunks, CHAIN, SUMS, ROWS, LANES), jnp.float32),
            pltpu.VMEM((chunks, CHAIN, SUMS, ROWS, LANES), jnp.float32),
            *(direct if whole else []),
        ],
        compiler_params=pltpu.CompilerParams(
            collective_id=0, has_side_effects=True, vmem_limit_bytes=44 * 2**20
        ),
        name="climatology",
    )(field)
    return pl.pallas_call(
        put_out,
        out_shape=tuple(jax.ShapeDtypeStruct(r.shape, r.dtype) for r in results),
        in_specs=[pl.BlockSpec(memory_space=pltpu.VMEM)] * 2,
        out_specs=(pl.BlockSpec(memory_space=pl.ANY),) * 2,
        scratch_shapes=[pltpu.SemaphoreType.DMA((2,))],
        compiler_params=pltpu.CompilerParams(vmem_limit_bytes=4 * 2**20),
        name="put_out",
    )(*results)


def solution(mesh):
    return jax.shard_map(
        local,
        mesh=mesh,
        in_specs=(P(("rep", "io"), None),),
        out_specs=(P("rep", None, "io"), P("rep", "io")),
        check_vma=False,
    )
```
